512 devices in a mesh: tm: 64 (over z_lo, y, core), strip: 8 (over z_hi, x).
Axes of the slice: x: 4, y: 8, z: 8 (z_hi: 2, z_lo: 4; z = z_hi * 4 + z_lo), core: 2. Of those that a mesh axis runs over, the one named last changes fastest.
Arguments:
- forward_u: float32 [64, 512, 1024], P('tm', 'strip'), may hold values from -4 to 4
- forward_v: float32 [64, 512, 1024], P('tm', 'strip'), may hold values from -4 to 4
- permittivity: float32 [512, 1024], P('strip'), may hold values from 1 to 3
- coarse_rate: float32 [64, 512, 1024], P('tm', 'strip'), may hold values from 0.2 to 8
- modulation: float32 [32], replicated, may hold values from 0 to 0.3
- tile_map: int32 [4, 8], replicated, may hold values from 0 to 31
- start_step: int32 [64], P('tm'), may hold values from 0 to 255
Outputs:
- adjoint_u: float32 [64, 512, 1024], P('tm', 'strip')
- adjoint_v: float32 [64, 512, 1024], P('tm', 'strip')
- depth_grad: float32 [32], replicated
The draws below stay inside these ranges and needn't reach their ends.
Inputs may be any that keep to these rules, and one draw needn't show every extreme that they name: `tile_map`: tile parameter indices. `start_step`: start steps within one period.
All inputs are finite; a program needn't handle non-finite values.
Results may differ from the reference program's by a relative error of at most 0.0003.
Values sent between devices are 32-bit elements; how exact they have to be, the bound alone decides.
No kernel may reach another device: no remote copies, remote signals or barrier semaphores. Data moves between devices by JAX's collectives and lax.ppermute only.
A program may use at most 128 MiB of HBM per device.

```python
import math
import jax
import jax.numpy as jnp
from jax import lax

NY = 1024
TILE = 128
STEPS = 2
STENCIL = 4
PERIOD = 256
PARAMS = 32
SLICES = 64
NX = 512
TX = 4
TY = 8


def touch_ends(entries, rng, smallest, top_value):
    longest = entries.shape.index(max(entries.shape))
    spots = []
    for shift in (0, 1):
        where = [jax.random.randint(jax.random.fold_in(rng, axis), (), 0, length) for axis, length in enumerate(entries.shape)]
        where[longest] = (where[longest] + shift) % entries.shape[longest]
        spots.append(tuple(where))
    return entries.at[spots[0]].set(smallest).at[spots[1]].set(top_value)


def levels(rng, shape, pieces, smallest, largest):
    def one(axis_at, parts):
        steps = jax.random.uniform(jax.random.fold_in(jax.random.fold_in(rng, 6), axis_at), (parts,), jnp.float32, smallest / len(pieces), largest / len(pieces))
        return jnp.repeat(jnp.exp(steps), shape[axis_at] // parts).reshape((-1,) + (1,) * (len(shape) - axis_at - 1))

    loudness = one(*pieces[0])
    for cut in pieces[1:]:
        loudness = loudness * one(*cut)
    return loudness


def centred(key, extent, spread, reach, split=(), held_as=jnp.bfloat16):
    entries = jax.random.normal(key, extent, jnp.float32) * spread
    if len(split) > 0:
        entries = levels(key, extent, split, -0.22, 0.18) * entries
    return jnp.clip(entries, min=-reach, max=reach).astype(held_as)


def setup_inputs(seed: int = 0) -> dict:
    seeds = jax.random.split(jax.random.key(seed), 8)
    forward_u = centred(seeds[0], (SLICES, NX, NY), 0.5, 4.0, ((0, 64), (1, 8)), jnp.float32)
    forward_v = centred(seeds[1], (SLICES, NX, NY), 0.5, 4.0, ((0, 64), (1, 8)), jnp.float32)
    permittivity = jnp.clip(1.0 + 2.0 * jax.random.uniform(seeds[2], (NX, NY), jnp.float32) ** levels(seeds[2], (NX, NY), ((0, 8),), -0.2, 0.2), 1.0, 3.0)
    coarse_rate = jnp.clip(jnp.exp(math.log(8.0) - 3.6888794 * jax.random.uniform(seeds[3], (SLICES, NX, NY), jnp.float32) ** levels(seeds[3], (SLICES, NX, NY), ((0, 64), (1, 8)), -0.2, 0.2)), 0.2, 8.0)
    modulation = jnp.clip(jax.random.uniform(seeds[4], (PARAMS,), jnp.float32, 0.0, 0.3), 0.0, 0.3)
    tile_map = touch_ends(jax.random.randint(seeds[5], (TX, TY), 0, PARAMS), jax.random.fold_in(seeds[5], 1), 0, PARAMS - 1).astype(jnp.int32)
    start_step = touch_ends(jax.random.randint(seeds[6], (SLICES,), 0, PERIOD), jax.random.fold_in(seeds[6], 1), 0, PERIOD - 1).astype(jnp.int32)
    return dict(forward_u=forward_u, forward_v=forward_v, permittivity=permittivity, coarse_rate=coarse_rate, modulation=modulation, tile_map=tile_map, start_step=start_step)


stencil_coef = (-205.0 / 72.0, 8.0 / 5.0, -1.0 / 5.0, 8.0 / 315.0, -1.0 / 560.0)
time_step = 0.4
damping_rate = 0.1


def laplacian_rows(padded, rim_width):
    row_count = padded.shape[0] - 2 * rim_width
    center = padded[rim_width:rim_width + row_count]
    summed = (2.0 * stencil_coef[0]) * center
    for offset in range(1, 5):
        along_x = padded[rim_width + offset:rim_width + offset + row_count] + padded[rim_width - offset:rim_width - offset + row_count]
        along_y = jnp.roll(center, offset, axis=1) + jnp.roll(center, -offset, axis=1)
        summed = summed + stencil_coef[offset] * (along_x + along_y)
    return summed


def pad_rows(field):
    return jnp.pad(field, ((STENCIL, STENCIL), (0, 0)))


def reference(forward_u, forward_v, permittivity, coarse_rate, modulation, tile_map, start_step):
    cell_depth = jnp.repeat(jnp.repeat(modulation[tile_map], TILE, axis=0), TILE, axis=1)

    def phases(start_index):
        offsets = (start_index + jnp.arange(STEPS, dtype=jnp.int32)).astype(jnp.float32)
        return jnp.cos((2.0 * jnp.pi / PERIOD) * offsets)

    def forward_run(field_u, field_v, cosines):
        forcings = []
        eps_all = []
        for level in range(STEPS):
            eps_now = permittivity * (1.0 + cell_depth * cosines[level])
            forcing = laplacian_rows(pad_rows(field_u), STENCIL) - damping_rate * field_v
            forcings.append(forcing)
            eps_all.append(eps_now)
            field_v = field_v + time_step * forcing / eps_now
            field_u = field_u + time_step * field_v
        return field_u, field_v, forcings, eps_all

    def forward_map(element):
        field_u, field_v, start_index = element
        end_u, end_v, forcings, eps_all = forward_run(field_u, field_v, phases(start_index))
        return end_u, end_v

    end_u, end_v = lax.map(forward_map, (forward_u, forward_v, start_step))
    mismatch_u = end_u - jnp.roll(forward_u, -1, axis=0)
    mismatch_v = end_v - jnp.roll(forward_v, -1, axis=0)
    retain = jnp.exp(-coarse_rate / SLICES)

    def compose(carried, element):
        cycle_a, cycle_bu, cycle_bv = carried
        factor, term_u, term_v = element
        return (factor * cycle_a, factor * cycle_bu + term_u, factor * cycle_bv + term_v), None

    ones = jnp.ones((NX, NY), jnp.float32)
    zeros = jnp.zeros((NX, NY), jnp.float32)
    (cycle_a, cycle_bu, cycle_bv), unused = lax.scan(compose, (ones, zeros, zeros), (retain, mismatch_u, mismatch_v), reverse=True)
    first_u = cycle_bu / (1.0 - cycle_a)
    first_v = cycle_bv / (1.0 - cycle_a)

    def backward(carried, element):
        factor, term_u, term_v = element
        coarse_u = factor * carried[0] + term_u
        coarse_v = factor * carried[1] + term_v
        return (coarse_u, coarse_v), (coarse_u, coarse_v)

    unused, (coarse_u, coarse_v) = lax.scan(backward, (first_u, first_v), (retain, mismatch_u, mismatch_v), reverse=True)

    def adjoint_map(element):
        field_u, field_v, back_u, back_v, start_index = element
        cosines = phases(start_index)
        end_u, end_v, forcings, eps_all = forward_run(field_u, field_v, cosines)
        gradient_cells = jnp.zeros((NX, NY), jnp.float32)
        for level in reversed(range(STEPS)):
            eps_now = eps_all[level]
            total_v = back_v + time_step * back_u
            weighted = (time_step / eps_now) * total_v
            back_u = back_u + laplacian_rows(pad_rows(weighted), STENCIL)
            back_v = (1.0 - time_step * damping_rate / eps_now) * total_v
            gradient_cells = gradient_cells - cosines[level] * time_step * total_v * forcings[level] / (eps_now * eps_now)
        cell_terms = gradient_cells * permittivity
        tile_sums = jnp.sum(cell_terms.reshape(NX // TILE, TILE, NY // TILE, TILE), axis=(1, 3))
        return back_u, back_v, tile_sums

    back_u, back_v, tile_sums = lax.map(adjoint_map, (forward_u, forward_v, coarse_u, coarse_v, start_step))
    adjoint_u = back_u - jnp.roll(coarse_u, 1, axis=0)
    adjoint_v = back_v - jnp.roll(coarse_v, 1, axis=0)
    tile_total = jnp.sum(tile_sums, axis=0)
    depth_grad = jax.ops.segment_sum(tile_total.reshape(-1), tile_map.reshape(-1).astype(jnp.int32), num_segments=PARAMS)
    return adjoint_u, adjoint_v, depth_grad
```

```python
import functools

import jax
import jax.numpy as jnp
from jax import lax
from jax.experimental import pallas as pl
from jax.experimental.pallas import tpu as pltpu
from jax.sharding import Mesh
from jax.sharding import PartitionSpec as P

TILE = 128
PERIOD = 256
STRIP = ("strip_0", "strip_1")
TM = ("tm_0", "tm_1", "tm_2")
CHIPS = ("tm_0", "tm_1")
CORE = "tm_2"
PAD = 8

COEF = (-205.0 / 72.0, 8.0 / 5.0, -1.0 / 5.0, 8.0 / 315.0, -1.0 / 560.0)
DT = 0.4
DAMP = 0.1

INTERPRET = False

VMEM = pl.BlockSpec(memory_space=pltpu.VMEM)
SMEM = pl.BlockSpec(memory_space=pltpu.SMEM)


def call(kernel, ins, outs, scratch=()):
    return pl.pallas_call(
        kernel,
        in_specs=ins,
        out_specs=[VMEM] * len(outs),
        out_shape=[jax.ShapeDtypeStruct(shape, jnp.float32) for shape in outs],
        scratch_shapes=[pltpu.VMEM(shape, jnp.float32) for shape in scratch],
        interpret=INTERPRET,
    )


def laplacian(frame, first, count):
    width = frame.shape[1]
    center = frame[first : first + count, :]
    summed = (2.0 * COEF[0]) * center
    for j in range(1, 5):
        rows = frame[first + j : first + j + count, :] + frame[first - j : first - j + count, :]
        cols = pltpu.roll(center, j, 1) + pltpu.roll(center, width - j, 1)
        summed = summed + COEF[j] * (rows + cols)
    return summed


def depth_row(modulation, tile_map, row, count):
    row = jnp.clip(row, 0, tile_map.shape[0] - 1)
    parts = [
        jnp.full((count, TILE), modulation[tile_map[row, j]], jnp.float32)
        for j in range(tile_map.shape[1])
    ]
    return jnp.concatenate(parts, axis=1)


def cosine(step, level):
    offset = jnp.full((8, 128), (step + level).astype(jnp.float32))
    return jnp.cos((2.0 * jnp.pi / PERIOD) * offset)[:1, :1]


def extended(lo, mid, hi):
    return jnp.concatenate([lo, mid, hi], axis=0)


def setting(place, step, modulation, tile_map, eps, lo, hi, rows, strips):
    strip = place[0] // 2
    first = strip * rows
    has_lo = strip > 0
    has_hi = strip < strips - 1
    width = eps.shape[1]
    static = extended(
        jnp.where(has_lo, lo, 1.0), eps, jnp.where(has_hi, hi, 1.0)
    )
    depth = extended(
        depth_row(modulation, tile_map, (first - 1) // TILE + jnp.where(has_lo, 0, 1), PAD),
        depth_row(modulation, tile_map, first // TILE, rows),
        depth_row(modulation, tile_map, (first + rows) // TILE, PAD),
    )
    cosines = [cosine(step[0], level) for level in range(2)]
    inverse = [1.0 / (static * (1.0 + depth * cosines[level])) for level in range(2)]

    def in_grid(cells):
        zero = jnp.zeros((PAD, width), jnp.float32)
        return extended(
            jnp.where(has_lo, cells[:PAD], zero),
            cells[PAD : PAD + rows],
            jnp.where(has_hi, cells[PAD + rows :], zero),
        )

    return cosines, inverse, in_grid


def fill(frame, cells):
    count, width = cells.shape
    frame[:PAD, :] = jnp.zeros((PAD, width), jnp.float32)
    frame[PAD : PAD + count, :] = cells
    frame[PAD + count : 2 * PAD + count, :] = jnp.zeros((PAD, width), jnp.float32)


def edges_kernel(u, v, eps, uv, top, bottom):
    rows = u.shape[0]
    uv[0] = u[...]
    uv[1] = v[...]
    for i, field in enumerate((u, v, eps)):
        top[i * PAD : (i + 1) * PAD, :] = field[:PAD, :]
        bottom[i * PAD : (i + 1) * PAD, :] = field[rows - PAD :, :]


def forward_kernel(
    slices, strips,
    place, step, modulation, tile_map, uv, eps, rate, lo, hi, following,
    keep, send, forcing_0, forcing_1, frame, whole,
):
    rows = eps.shape[0]
    cosines, inverse, in_grid = setting(
        place, step, modulation, tile_map, eps[...],
        lo[2 * PAD :, :], hi[2 * PAD :, :], rows, strips,
    )
    count = rows + 2 * PAD
    u = extended(lo[:PAD, :], uv[0], hi[:PAD, :])
    v = extended(lo[PAD : 2 * PAD, :], uv[1], hi[PAD : 2 * PAD, :])
    fill(frame, u)
    force = laplacian(frame, PAD, count) - DAMP * v
    forcing_0[...] = force
    v = v + DT * force * inverse[0]
    u = in_grid(u + DT * v)
    fill(frame, u)
    v = v[PAD : PAD + rows]
    u = u[PAD : PAD + rows]
    force = laplacian(frame, 2 * PAD, rows) - DAMP * v
    forcing_1[...] = force
    v = v + DT * force * inverse[1][PAD : PAD + rows]
    u = u + DT * v
    whole[0] = jnp.exp(-rate[...] / slices)
    whole[1] = u - following[0]
    whole[2] = v - following[1]
    core = place[0] % 2
    half = rows // 2
    for i in range(3):
        keep[i] = whole[i, pl.ds(pl.multiple_of(core * half, half), half), :]
        send[i] = whole[i, pl.ds(pl.multiple_of((1 - core) * half, half), half), :]


def blocks(rows, width):
    return [(8 * i, 128 * j) for i in range(rows // 8) for j in range(width // 128)]


def pair_kernel(place, keep, came, out):
    first = place[0] % 2 == 0
    half, width = keep.shape[1:]
    for t, (r, c) in enumerate(blocks(half, width)):
        mine = [keep[i, r : r + 8, c : c + 128] for i in range(3)]
        other = [came[i, r : r + 8, c : c + 128] for i in range(3)]
        a, bu, bv = [jnp.where(first, m, o) for m, o in zip(mine, other)]
        a_next, bu_next, bv_next = [jnp.where(first, o, m) for m, o in zip(mine, other)]
        out[t, 0:8, :] = a * a_next
        out[t, 8:16, :] = a * bu_next + bu
        out[t, 16:24, :] = a * bv_next + bv


def cycle_kernel(maps, carries):
    pairs, held = maps.shape[:2]
    for t in range(held):
        a = maps[pairs - 1, t, 0:8, :]
        bu = maps[pairs - 1, t, 8:16, :]
        bv = maps[pairs - 1, t, 16:24, :]
        for p in reversed(range(pairs - 1)):
            factor = maps[p, t, 0:8, :]
            a = factor * a
            bu = factor * bu + maps[p, t, 8:16, :]
            bv = factor * bv + maps[p, t, 16:24, :]
        share = 1.0 / (1.0 - a)
        u = bu * share
        v = bv * share
        for p in reversed(range(pairs)):
            carries[p, t, 0:8, :] = u
            carries[p, t, 8:16, :] = v
            if p:
                factor = maps[p, t, 0:8, :]
                u = factor * u + maps[p, t, 8:16, :]
                v = factor * v + maps[p, t, 16:24, :]


def spread_kernel(place, carries, keep, came, mine, send):
    first = place[0] % 2 == 0
    half, width = keep.shape[1:]
    for t, (r, c) in enumerate(blocks(half, width)):
        own = [keep[i, r : r + 8, c : c + 128] for i in range(3)]
        other = [came[i, r : r + 8, c : c + 128] for i in range(3)]
        early = [jnp.where(first, m, o) for m, o in zip(own, other)]
        late = [jnp.where(first, o, m) for m, o in zip(own, other)]
        for i in range(2):
            entering = carries[t, 8 * i : 8 * i + 8, :]
            late_state = late[0] * entering + late[1 + i]
            early_state = early[0] * late_state + early[1 + i]
            mine[i, r : r + 8, c : c + 128] = jnp.where(first, early_state, late_state)
            send[i, r : r + 8, c : c + 128] = jnp.where(first, late_state, early_state)


def join_kernel(place, mine, came, coarse, top, bottom):
    core = place[0] % 2
    half = mine.shape[1]
    rows = 2 * half
    for i in range(2):
        coarse[i, pl.ds(pl.multiple_of(core * half, half), half), :] = mine[i]
        coarse[i, pl.ds(pl.multiple_of((1 - core) * half, half), half), :] = came[i]
    for i in range(2):
        top[i * PAD : (i + 1) * PAD, :] = coarse[i, :PAD, :]
        bottom[i * PAD : (i + 1) * PAD, :] = coarse[i, rows - PAD :, :]


def adjoint_kernel(
    strips,
    place, step, modulation, tile_map, coarse, coarse_lo, coarse_hi, eps, lo, hi,
    forcing_0, forcing_1, preceding,
    adjoint_u, adjoint_v, partial, frame,
):
    rows, width = eps.shape
    cosines, inverse, in_grid = setting(
        place, step, modulation, tile_map, eps[...],
        lo[2 * PAD :, :], hi[2 * PAD :, :], rows, strips,
    )
    count = rows + 2 * PAD
    inner = slice(PAD, PAD + rows)
    u = extended(coarse_lo[:PAD, :], coarse[0], coarse_hi[:PAD, :])
    v = extended(coarse_lo[PAD:, :], coarse[1], coarse_hi[PAD:, :])
    total = v + DT * u
    fill(frame, (DT * inverse[1]) * total)
    u = u + laplacian(frame, PAD, count)
    v = (1.0 - (DT * DAMP) * inverse[1]) * total
    cells = (cosines[1] * DT) * total[inner] * forcing_1[...] * (inverse[1] * inverse[1])[inner]
    total = v + DT * u
    fill(frame, in_grid((DT * inverse[0]) * total))
    total = total[inner]
    inverse_0 = inverse[0][inner]
    cells = cells + (cosines[0] * DT) * total * forcing_0[inner, :] * (inverse_0 * inverse_0)
    adjoint_u[...] = u[inner] + laplacian(frame, 2 * PAD, rows) - preceding[0]
    adjoint_v[...] = (1.0 - (DT * DAMP) * inverse_0) * total - preceding[1]
    column = jnp.sum(cells * eps[...], axis=0, keepdims=True)
    row = (place[0] // 2) * rows // TILE
    lanes = lax.broadcasted_iota(jnp.int32, (1, 128), 1)
    gradient = jnp.zeros((1, 128), jnp.float32)
    for j in range(width // TILE):
        amount = jnp.sum(column[:, j * TILE : (j + 1) * TILE], axis=1, keepdims=True)
        gradient = gradient - jnp.where(lanes == tile_map[row, j], amount, 0.0)
    partial[...] = gradient


def shifted(array, axis, by):
    length = lax.axis_size(axis)
    return lax.ppermute(array, axis, [(i, (i + by) % length) for i in range(length)])


def both_ways(top, bottom):
    length = lax.axis_size(STRIP)
    lo = lax.ppermute(bottom, STRIP, [(i, i + 1) for i in range(length - 1)])
    hi = lax.ppermute(top, STRIP, [(i + 1, i) for i in range(length - 1)])
    return lo, hi


def summed(array, axes):
    count = lax.axis_size(axes)
    copies = jnp.broadcast_to(array[None], (count,) + array.shape)
    pieces = lax.all_to_all(copies, axes, 0, 0, tiled=True)
    return jnp.sum(pieces, axis=0)


def shards(forward_u, forward_v, permittivity, coarse_rate, modulation, tile_map, start_step):
    rows, width = permittivity.shape
    half = rows // 2
    strips = lax.axis_size(STRIP)
    slices = lax.axis_size(TM)
    pairs = lax.axis_size(CHIPS)
    tiles = half // 8 * (width // 128)
    held = tiles // pairs
    place = (2 * lax.axis_index(STRIP) + lax.axis_index(CORE)).astype(jnp.int32).reshape(1)
    field = (rows, width)
    edge = (3 * PAD, width)
    scalars = [SMEM] * 4
    frame = (rows + 4 * PAD, width)

    uv, top, bottom = call(edges_kernel, [VMEM] * 3, [(2,) + field, edge, edge])(
        forward_u[0], forward_v[0], permittivity
    )
    following = shifted(uv, TM, -1)
    lo, hi = both_ways(top, bottom)
    keep, send, forcing_0, forcing_1 = call(
        functools.partial(forward_kernel, slices, strips),
        scalars + [VMEM] * 6,
        [(3, half, width), (3, half, width), (rows + 2 * PAD, width), field],
        [frame, (3,) + field],
    )(place, start_step, modulation, tile_map, uv, permittivity, coarse_rate[0], lo, hi, following)

    came = shifted(send, CORE, 1)
    (maps,) = call(pair_kernel, [SMEM, VMEM, VMEM], [(tiles, 24, 128)])(place, keep, came)
    maps = lax.all_to_all(maps.reshape(pairs, held * 24, 128), CHIPS, 0, 0, tiled=True)
    (carries,) = call(cycle_kernel, [VMEM], [(pairs, held, 16, 128)])(
        maps.reshape(pairs, held, 24, 128)
    )
    carries = lax.all_to_all(carries.reshape(pairs, held * 16, 128), CHIPS, 0, 0, tiled=True)
    mine, send = call(spread_kernel, [SMEM] + [VMEM] * 3, [(2, half, width)] * 2)(
        place, carries.reshape(tiles, 16, 128), keep, came
    )
    edge = (2 * PAD, width)
    coarse, top, bottom = call(join_kernel, [SMEM, VMEM, VMEM], [(2,) + field, edge, edge])(
        place, mine, shifted(send, CORE, 1)
    )
    preceding = shifted(coarse, TM, 1)
    coarse_lo, coarse_hi = both_ways(top, bottom)
    adjoint_u, adjoint_v, partial = call(
        functools.partial(adjoint_kernel, strips),
        scalars + [VMEM] * 9,
        [field, field, (1, 128)],
        [frame],
    )(
        place, start_step, modulation, tile_map, coarse, coarse_lo, coarse_hi,
        permittivity, lo, hi, forcing_0, forcing_1, preceding,
    )
    total = summed(summed(partial, TM), STRIP)
    depth_grad = total[0, : modulation.shape[0]]
    return (adjoint_u[None], adjoint_v[None], depth_grad)


def solution(mesh):
    torus = Mesh(
        mesh.devices.reshape(4, 8, 2, 2, 4), ("tm_0", "tm_1", "tm_2", "strip_0", "strip_1")
    )
    return on_torus(torus)


def on_torus(torus):
    placed = (
        P(TM, STRIP, None),
        P(TM, STRIP, None),
        P(STRIP, None),
        P(TM, STRIP, None),
        P(),
        P(),
        P(TM),
    )
    return jax.shard_map(
        shards,
        mesh=torus,
        in_specs=placed,
        out_specs=(P(TM, STRIP, None), P(TM, STRIP, None), P()),
        check_vma=False,
    )
```

```python
import functools

import jax
import jax.numpy as jnp
from jax import lax
from jax.experimental import pallas as pl
from jax.experimental.pallas import tpu as pltpu
from jax.sharding import Mesh
from jax.sharding import PartitionSpec as P

TILE = 128
PERIOD = 256
STRIP = ("strip_0", "strip_1")
TM = ("tm_0", "tm_1", "tm_2")
CHIPS = ("tm_0", "tm_1")
CORE = "tm_2"
PAD = 8

COEF = (-205.0 / 72.0, 8.0 / 5.0, -1.0 / 5.0, 8.0 / 315.0, -1.0 / 560.0)
DT = 0.4
DAMP = 0.1

INTERPRET = False
VMEM_LIMIT = 12 * 1024 * 1024

VMEM = pl.BlockSpec(memory_space=pltpu.VMEM)
SMEM = pl.BlockSpec(memory_space=pltpu.SMEM)


def call(kernel, ins, outs, scratch=()):
    return pl.pallas_call(
        kernel,
        in_specs=ins,
        out_specs=[VMEM] * len(outs),
        out_shape=[jax.ShapeDtypeStruct(shape, jnp.float32) for shape in outs],
        scratch_shapes=[pltpu.VMEM(shape, jnp.float32) for shape in scratch],
        compiler_params=pltpu.CompilerParams(vmem_limit_bytes=VMEM_LIMIT),
        interpret=INTERPRET,
    )


def laplacian(frame, first, count):
    width = frame.shape[1]
    center = frame[first : first + count, :]
    summed = (2.0 * COEF[0]) * center
    for j in range(1, 5):
        rows = frame[first + j : first + j + count, :] + frame[first - j : first - j + count, :]
        cols = pltpu.roll(center, j, 1) + pltpu.roll(center, width - j, 1)
        summed = summed + COEF[j] * (rows + cols)
    return summed


def depth_row(modulation, tile_map, row, count):
    row = jnp.clip(row, 0, tile_map.shape[0] - 1)
    parts = [
        jnp.full((count, TILE), modulation[tile_map[row, j]], jnp.float32)
        for j in range(tile_map.shape[1])
    ]
    return jnp.concatenate(parts, axis=1)


def cosine(step, level):
    offset = jnp.full((8, 128), (step + level).astype(jnp.float32))
    return jnp.cos((2.0 * jnp.pi / PERIOD) * offset)[:1, :1]


def extended(lo, mid, hi):
    return jnp.concatenate([lo, mid, hi], axis=0)


def setting(place, step, modulation, tile_map, eps, lo, hi, rows, strips):
    strip = place[0] // 2
    first = strip * rows
    has_lo = strip > 0
    has_hi = strip < strips - 1
    width = eps.shape[1]
    static = extended(
        jnp.where(has_lo, lo, 1.0), eps, jnp.where(has_hi, hi, 1.0)
    )
    depth = extended(
        depth_row(modulation, tile_map, (first - 1) // TILE + jnp.where(has_lo, 0, 1), PAD),
        depth_row(modulation, tile_map, first // TILE, rows),
        depth_row(modulation, tile_map, (first + rows) // TILE, PAD),
    )
    cosines = [cosine(step[0], level) for level in range(2)]
    inverse = [1.0 / (static * (1.0 + depth * cosines[level])) for level in range(2)]

    def in_grid(cells):
        zero = jnp.zeros((PAD, width), jnp.float32)
        return extended(
            jnp.where(has_lo, cells[:PAD], zero),
            cells[PAD : PAD + rows],
            jnp.where(has_hi, cells[PAD + rows :], zero),
        )

    return cosines, inverse, in_grid


def fill(frame, cells):
    count, width = cells.shape
    frame[:PAD, :] = jnp.zeros((PAD, width), jnp.float32)
    frame[PAD : PAD + count, :] = cells
    frame[PAD + count : 2 * PAD + count, :] = jnp.zeros((PAD, width), jnp.float32)


def edges_kernel(u, v, eps, uv, top, bottom):
    rows = u.shape[0]
    uv[0] = u[...]
    uv[1] = v[...]
    for i, field in enumerate((u, v, eps)):
        top[i * PAD : (i + 1) * PAD, :] = field[:PAD, :]
        bottom[i * PAD : (i + 1) * PAD, :] = field[rows - PAD :, :]


def forward_kernel(
    slices, strips,
    place, step, modulation, tile_map, uv, eps, rate, lo, hi, following,
    keep, send, forcing_0, forcing_1, frame, whole,
):
    rows = eps.shape[0]
    cosines, inverse, in_grid = setting(
        place, step, modulation, tile_map, eps[...],
        lo[2 * PAD :, :], hi[2 * PAD :, :], rows, strips,
    )
    count = rows + 2 * PAD
    u = extended(lo[:PAD, :], uv[0], hi[:PAD, :])
    v = extended(lo[PAD : 2 * PAD, :], uv[1], hi[PAD : 2 * PAD, :])
    fill(frame, u)
    force = laplacian(frame, PAD, count) - DAMP * v
    forcing_0[...] = force
    v = v + DT * force * inverse[0]
    u = in_grid(u + DT * v)
    fill(frame, u)
    v = v[PAD : PAD + rows]
    u = u[PAD : PAD + rows]
    force = laplacian(frame, 2 * PAD, rows) - DAMP * v
    forcing_1[...] = force
    v = v + DT * force * inverse[1][PAD : PAD + rows]
    u = u + DT * v
    whole[0] = jnp.exp(-rate[...] / slices)
    whole[1] = u - following[0]
    whole[2] = v - following[1]
    core = place[0] % 2
    half = rows // 2
    for i in range(3):
        keep[i] = whole[i, pl.ds(pl.multiple_of(core * half, half), half), :]
        send[i] = whole[i, pl.ds(pl.multiple_of((1 - core) * half, half), half), :]


def blocks(rows, width):
    return [(8 * i, 128 * j) for i in range(rows // 8) for j in range(width // 128)]


def pair_kernel(place, keep, came, out):
    first = place[0] % 2 == 0
    half, width = keep.shape[1:]
    for t, (r, c) in enumerate(blocks(half, width)):
        mine = [keep[i, r : r + 8, c : c + 128] for i in range(3)]
        other = [came[i, r : r + 8, c : c + 128] for i in range(3)]
        a, bu, bv = [jnp.where(first, m, o) for m, o in zip(mine, other)]
        a_next, bu_next, bv_next = [jnp.where(first, o, m) for m, o in zip(mine, other)]
        out[t, 0:8, :] = a * a_next
        out[t, 8:16, :] = a * bu_next + bu
        out[t, 16:24, :] = a * bv_next + bv


def cycle_kernel(maps, carries):
    pairs, held = maps.shape[:2]
    for t in range(held):
        a = maps[pairs - 1, t, 0:8, :]
        bu = maps[pairs - 1, t, 8:16, :]
        bv = maps[pairs - 1, t, 16:24, :]
        for p in reversed(range(pairs - 1)):
            factor = maps[p, t, 0:8, :]
            a = factor * a
            bu = factor * bu + maps[p, t, 8:16, :]
            bv = factor * bv + maps[p, t, 16:24, :]
        share = 1.0 / (1.0 - a)
        u = bu * share
        v = bv * share
        for p in reversed(range(pairs)):
            carries[p, t, 0:8, :] = u
            carries[p, t, 8:16, :] = v
            if p:
                factor = maps[p, t, 0:8, :]
                u = factor * u + maps[p, t, 8:16, :]
                v = factor * v + maps[p, t, 16:24, :]


def spread_kernel(place, carries, keep, came, mine, send):
    first = place[0] % 2 == 0
    half, width = keep.shape[1:]
    for t, (r, c) in enumerate(blocks(half, width)):
        own = [keep[i, r : r + 8, c : c + 128] for i in range(3)]
        other = [came[i, r : r + 8, c : c + 128] for i in range(3)]
        early = [jnp.where(first, m, o) for m, o in zip(own, other)]
        late = [jnp.where(first, o, m) for m, o in zip(own, other)]
        for i in range(2):
            entering = carries[t, 8 * i : 8 * i + 8, :]
            late_state = late[0] * entering + late[1 + i]
            early_state = early[0] * late_state + early[1 + i]
            mine[i, r : r + 8, c : c + 128] = jnp.where(first, early_state, late_state)
            send[i, r : r + 8, c : c + 128] = jnp.where(first, late_state, early_state)


def join_kernel(place, mine, came, coarse, top, bottom):
    core = place[0] % 2
    half = mine.shape[1]
    rows = 2 * half
    for i in range(2):
        coarse[i, pl.ds(pl.multiple_of(core * half, half), half), :] = mine[i]
        coarse[i, pl.ds(pl.multiple_of((1 - core) * half, half), half), :] = came[i]
    for i in range(2):
        top[i * PAD : (i + 1) * PAD, :] = coarse[i, :PAD, :]
        bottom[i * PAD : (i + 1) * PAD, :] = coarse[i, rows - PAD :, :]


def adjoint_kernel(
    strips,
    place, step, modulation, tile_map, coarse, coarse_lo, coarse_hi, eps, lo, hi,
    forcing_0, forcing_1, preceding,
    adjoint_u, adjoint_v, partial, frame,
):
    rows, width = eps.shape
    cosines, inverse, in_grid = setting(
        place, step, modulation, tile_map, eps[...],
        lo[2 * PAD :, :], hi[2 * PAD :, :], rows, strips,
    )
    count = rows + 2 * PAD
    inner = slice(PAD, PAD + rows)
    u = extended(coarse_lo[:PAD, :], coarse[0], coarse_hi[:PAD, :])
    v = extended(coarse_lo[PAD:, :], coarse[1], coarse_hi[PAD:, :])
    total = v + DT * u
    fill(frame, (DT * inverse[1]) * total)
    u = u + laplacian(frame, PAD, count)
    v = (1.0 - (DT * DAMP) * inverse[1]) * total
    cells = (cosines[1] * DT) * total[inner] * forcing_1[...] * (inverse[1] * inverse[1])[inner]
    total = v + DT * u
    fill(frame, in_grid((DT * inverse[0]) * total))
    total = total[inner]
    inverse_0 = inverse[0][inner]
    cells = cells + (cosines[0] * DT) * total * forcing_0[inner, :] * (inverse_0 * inverse_0)
    adjoint_u[...] = u[inner] + laplacian(frame, 2 * PAD, rows) - preceding[0]
    adjoint_v[...] = (1.0 - (DT * DAMP) * inverse_0) * total - preceding[1]
    column = jnp.sum(cells * eps[...], axis=0, keepdims=True)
    row = (place[0] // 2) * rows // TILE
    lanes = lax.broadcasted_iota(jnp.int32, (1, 128), 1)
    gradient = jnp.zeros((1, 128), jnp.float32)
    for j in range(width // TILE):
        amount = jnp.sum(column[:, j * TILE : (j + 1) * TILE], axis=1, keepdims=True)
        gradient = gradient - jnp.where(lanes == tile_map[row, j], amount, 0.0)
    partial[...] = gradient


def shifted(array, axis, by):
    length = lax.axis_size(axis)
    return lax.ppermute(array, axis, [(i, (i + by) % length) for i in range(length)])


def both_ways(top, bottom):
    length = lax.axis_size(STRIP)
    lo = lax.ppermute(bottom, STRIP, [(i, i + 1) for i in range(length - 1)])
    hi = lax.ppermute(top, STRIP, [(i + 1, i) for i in range(length - 1)])
    return lo, hi


def summed(array, axes):
    count = lax.axis_size(axes)
    copies = jnp.broadcast_to(array[None], (count,) + array.shape)
    pieces = lax.all_to_all(copies, axes, 0, 0, tiled=True)
    return jnp.sum(pieces, axis=0)


def shards(forward_u, forward_v, permittivity, coarse_rate, modulation, tile_map, start_step):
    rows, width = permittivity.shape
    half = rows // 2
    strips = lax.axis_size(STRIP)
    slices = lax.axis_size(TM)
    pairs = lax.axis_size(CHIPS)
    tiles = half // 8 * (width // 128)
    held = tiles // pairs
    place = (2 * lax.axis_index(STRIP) + lax.axis_index(CORE)).astype(jnp.int32).reshape(1)
    field = (rows, width)
    edge = (3 * PAD, width)
    scalars = [SMEM] * 4
    frame = (rows + 4 * PAD, width)

    uv, top, bottom = call(edges_kernel, [VMEM] * 3, [(2,) + field, edge, edge])(
        forward_u[0], forward_v[0], permittivity
    )
    following = shifted(uv, TM, -1)
    lo, hi = both_ways(top, bottom)
    keep, send, forcing_0, forcing_1 = call(
        functools.partial(forward_kernel, slices, strips),
        scalars + [VMEM] * 6,
        [(3, half, width), (3, half, width), (rows + 2 * PAD, width), field],
        [frame, (3,) + field],
    )(place, start_step, modulation, tile_map, uv, permittivity, coarse_rate[0], lo, hi, following)

    came = shifted(send, CORE, 1)
    (maps,) = call(pair_kernel, [SMEM, VMEM, VMEM], [(tiles, 24, 128)])(place, keep, came)
    maps = lax.all_to_all(maps.reshape(pairs, held * 24, 128), CHIPS, 0, 0, tiled=True)
    (carries,) = call(cycle_kernel, [VMEM], [(pairs, held, 16, 128)])(
        maps.reshape(pairs, held, 24, 128)
    )
    carries = lax.all_to_all(carries.reshape(pairs, held * 16, 128), CHIPS, 0, 0, tiled=True)
    mine, send = call(spread_kernel, [SMEM] + [VMEM] * 3, [(2, half, width)] * 2)(
        place, carries.reshape(tiles, 16, 128), keep, came
    )
    edge = (2 * PAD, width)
    coarse, top, bottom = call(join_kernel, [SMEM, VMEM, VMEM], [(2,) + field, edge, edge])(
        place, mine, shifted(send, CORE, 1)
    )
    preceding = shifted(coarse, TM, 1)
    coarse_lo, coarse_hi = both_ways(top, bottom)
    adjoint_u, adjoint_v, partial = call(
        functools.partial(adjoint_kernel, strips),
        scalars + [VMEM] * 9,
        [field, field, (1, 128)],
        [frame],
    )(
        place, start_step, modulation, tile_map, coarse, coarse_lo, coarse_hi,
        permittivity, lo, hi, forcing_0, forcing_1, preceding,
    )
    total = summed(summed(partial, TM), STRIP)
    depth_grad = total[0, : modulation.shape[0]]
    return (adjoint_u[None], adjoint_v[None], depth_grad)


def solution(mesh):
    torus = Mesh(
        mesh.devices.reshape(4, 8, 2, 2, 4), ("tm_0", "tm_1", "tm_2", "strip_0", "strip_1")
    )
    return on_torus(torus)


def on_torus(torus):
    placed = (
        P(TM, STRIP, None),
        P(TM, STRIP, None),
        P(STRIP, None),
        P(TM, STRIP, None),
        P(),
        P(),
        P(TM),
    )
    return jax.shard_map(
        shards,
        mesh=torus,
        in_specs=placed,
        out_specs=(P(TM, STRIP, None), P(TM, STRIP, None), P()),
        check_vma=False,
    )
```

```python
import functools

import jax
import jax.numpy as jnp
from jax import lax
from jax.experimental import pallas as pl
from jax.experimental.pallas import tpu as pltpu
from jax.sharding import Mesh
from jax.sharding import PartitionSpec as P

TILE = 128
PERIOD = 256
STRIP = ("strip_0", "strip_1")
TM = ("tm_0", "tm_1", "tm_2")
CHIPS = ("tm_0", "tm_1")
CORE = "tm_2"
PAD = 8

COEF = (-205.0 / 72.0, 8.0 / 5.0, -1.0 / 5.0, 8.0 / 315.0, -1.0 / 560.0)
DT = 0.4
DAMP = 0.1

INTERPRET = False
VMEM_LIMIT = 12 * 1024 * 1024

HALVES = (CORE,) + STRIP
VMEM = pl.BlockSpec(memory_space=pltpu.VMEM)
SMEM = pl.BlockSpec(memory_space=pltpu.SMEM)
HBM = pl.BlockSpec(memory_space=pltpu.HBM)


def held(shape):
    return pltpu.VMEM(shape, jnp.float32) if isinstance(shape, tuple) else shape


def call(kernel, ins, outs, scratch=()):
    return pl.pallas_call(
        kernel,
        in_specs=ins,
        out_specs=[VMEM] * len(outs),
        out_shape=[jax.ShapeDtypeStruct(shape, jnp.float32) for shape in outs],
        scratch_shapes=[held(shape) for shape in scratch],
        compiler_params=pltpu.CompilerParams(vmem_limit_bytes=VMEM_LIMIT),
        interpret=INTERPRET,
    )


def laplacian(frame, first, count):
    width = frame.shape[1]
    center = frame[first : first + count, :]
    summed = (2.0 * COEF[0]) * center
    for j in range(1, 5):
        rows = frame[first + j : first + j + count, :] + frame[first - j : first - j + count, :]
        cols = pltpu.roll(center, j, 1) + pltpu.roll(center, width - j, 1)
        summed = summed + COEF[j] * (rows + cols)
    return summed


def depth_row(modulation, tile_map, row, count):
    row = jnp.clip(row, 0, tile_map.shape[0] - 1)
    parts = [
        jnp.full((count, TILE), modulation[tile_map[row, j]], jnp.float32)
        for j in range(tile_map.shape[1])
    ]
    return jnp.concatenate(parts, axis=1)


def depth_rows(modulation, tile_map, first, rows):
    return jnp.concatenate(
        [
            depth_row(modulation, tile_map, (first + TILE - 1) // TILE - 1, PAD),
            depth_row(modulation, tile_map, first // TILE, rows),
            depth_row(modulation, tile_map, (first + rows) // TILE, PAD),
        ],
        axis=0,
    )


def cosine(step, level):
    offset = jnp.broadcast_to(step + float(level), (8, 128))
    return jnp.cos((2.0 * jnp.pi / PERIOD) * offset)[:1, :1]


def place_of(place):
    return place[0] // 2, place[0] % 2


def at(start, count):
    return pl.ds(pl.multiple_of(start, PAD), count)


def gather_kernel(place, step, u, v, rate, out, sems):
    strip, core = place_of(place)
    count = u.shape[0] // 2 + PAD
    rows = at((count - 2 * PAD) * (1 - core), count)
    copies = [
        pltpu.make_async_copy(field.at[rows, :], out.at[pl.ds(count * i, count), :], sems.at[i])
        for i, field in enumerate((u, v, rate))
    ]
    for copy in copies:
        copy.start()
    tail = out.shape[0] - 3 * count
    out[3 * count :, :] = jnp.full((tail, out.shape[1]), step[0].astype(jnp.float32))
    for copy in copies:
        copy.wait()


def sort_kernel(place, u, v, rate, eps, came, state, early, edge):
    strip, core = place_of(place)
    half = u.shape[0] // 2
    count = half + PAD
    rows = at((half - PAD) * core, count)
    for i, field in enumerate((u, v, rate)):
        state[core, i] = field[rows, :]
        state[1 - core, i] = came[count * i : count * i + count, :]
    for i in range(2):
        early[i] = state[0, i, at(PAD * core, half), :]
    for k in range(2):
        for i in range(2):
            row = PAD * (2 * k + i)
            edge[row : row + PAD, :] = state[k, i, at(half * core, PAD), :]
    edge[4 * PAD :, :] = eps[at((2 * half - PAD) * core, PAD), :]


def forward_kernel(
    slices, strips,
    place, step, modulation, tile_map, state, eps, came, edge, following,
    maps, keep, near, far, inner,
    frame, field, static,
):
    strip, core = place_of(place)
    half = eps.shape[0] // 2
    width = eps.shape[1]
    rows = half + 2 * PAD
    first = (2 * strip + core) * half
    line = lax.broadcasted_iota(jnp.int32, (rows, width), 0)
    lowest = jnp.where(first > 0, 0, PAD)
    highest = jnp.where(first + half < strips * 2 * half, rows, half + PAD)
    in_grid = jnp.logical_and(line >= lowest, line < highest)
    body = at(PAD * (1 - core), half + PAD)
    rim = at((half + PAD) * core, PAD)

    static[body, :] = eps[at((half - PAD) * core, half + PAD), :]
    static[rim, :] = edge[4 * PAD :, :]
    steady = jnp.where(in_grid, static[...], 1.0)
    depth = depth_rows(modulation, tile_map, first, half)
    mid = slice(PAD, PAD + half)
    own = jnp.full((1, 1), step[0].astype(jnp.float32))
    other = came[came.shape[0] - 1 :, :1]
    for k in range(2):
        start = jnp.where(core == k, own, other)
        cosines = [cosine(start, level) for level in range(2)]
        inverse = [1.0 / (steady * (1.0 + depth * cosines[level])) for level in range(2)]
        for i in range(2):
            field[i, body, :] = state[k, i]
            field[i, rim, :] = edge[PAD * (2 * k + i) : PAD * (2 * k + i) + PAD, :]
        u = field[0]
        v = field[1]
        frame[:PAD, :] = jnp.zeros((PAD, width), jnp.float32)
        frame[PAD + rows :, :] = jnp.zeros((PAD, width), jnp.float32)
        frame[PAD : PAD + rows, :] = u
        force = laplacian(frame, PAD, rows) - DAMP * v
        weight = (cosines[0] * -DT) * force * (inverse[0] * inverse[0]) * steady
        far[k] = jnp.where(in_grid, weight, 0.0)
        v = v + DT * force * inverse[0]
        u = jnp.where(in_grid, u + DT * v, 0.0)
        frame[PAD : PAD + rows, :] = u
        v = v[mid]
        u = u[mid]
        force = laplacian(frame, 2 * PAD, half) - DAMP * v
        late = inverse[1][mid]
        near[k] = (cosines[1] * -DT) * force * (late * late) * steady[mid]
        inner[k] = late
        v = v + DT * force * late
        u = u + DT * v
        keep[k, 0] = jnp.exp(-state[k, 2, at(PAD * core, half), :] / slices)
        if k == 0:
            keep[0, 1] = u - state[1, 0, at(PAD * core, half), :]
            keep[0, 2] = v - state[1, 1, at(PAD * core, half), :]
        else:
            keep[1, 1] = u - following[0]
            keep[1, 2] = v - following[1]
    for t, (r, c) in enumerate(blocks(half, width)):
        a, bu, bv = [keep[0, i, r : r + 8, c : c + 128] for i in range(3)]
        a_next, bu_next, bv_next = [keep[1, i, r : r + 8, c : c + 128] for i in range(3)]
        maps[t, 0:8, :] = a * a_next
        maps[t, 8:16, :] = a * bu_next + bu
        maps[t, 16:24, :] = a * bv_next + bv


def blocks(rows, width):
    return [(8 * i, 128 * j) for i in range(rows // 8) for j in range(width // 128)]


def cycle_kernel(maps, carries):
    pairs, held = maps.shape[:2]
    for t in range(held):
        a = maps[pairs - 1, t, 0:8, :]
        bu = maps[pairs - 1, t, 8:16, :]
        bv = maps[pairs - 1, t, 16:24, :]
        for p in reversed(range(pairs - 1)):
            factor = maps[p, t, 0:8, :]
            a = factor * a
            bu = factor * bu + maps[p, t, 8:16, :]
            bv = factor * bv + maps[p, t, 16:24, :]
        share = 1.0 / (1.0 - a)
        u = bu * share
        v = bv * share
        for p in reversed(range(pairs)):
            carries[p, t, 0:8, :] = u
            carries[p, t, 8:16, :] = v
            if p:
                factor = maps[p, t, 0:8, :]
                u = factor * u + maps[p, t, 8:16, :]
                v = factor * v + maps[p, t, 16:24, :]


def add_tiles(gradient, tile_map, row, column):
    lanes = lax.broadcasted_iota(jnp.int32, (1, 128), 1)
    row = jnp.clip(row, 0, tile_map.shape[0] - 1)
    for j in range(tile_map.shape[1]):
        amount = jnp.sum(column[:, j * TILE : (j + 1) * TILE], axis=1, keepdims=True)
        gradient = gradient + jnp.where(lanes == tile_map[row, j], amount, 0.0)
    return gradient


def spread_kernel(
    place, tile_map, carries, keep, near, far, inner,
    coarse, late, edge, partial, frame,
):
    strip, core = place_of(place)
    half, width = keep.shape[2:]
    rows = half + 2 * PAD
    first = (2 * strip + core) * half
    for t, (r, c) in enumerate(blocks(half, width)):
        for i in range(2):
            entering = carries[t, 8 * i : 8 * i + 8, :]
            for k in (1, 0):
                entering = (
                    keep[k, 0, r : r + 8, c : c + 128] * entering
                    + keep[k, 1 + i, r : r + 8, c : c + 128]
                )
                coarse[k, i, r : r + 8, c : c + 128] = entering
    frame[...] = jnp.zeros_like(frame)
    above = jnp.zeros((1, width), jnp.float32)
    amid = jnp.zeros((1, width), jnp.float32)
    below = jnp.zeros((1, width), jnp.float32)
    for k in range(2):
        for i in range(2):
            late[i] = coarse[1, i]
            row = PAD * (2 * k + i)
            edge[row : row + PAD, :] = coarse[k, i, at((half - PAD) * core, PAD), :]
        u = coarse[k, 0]
        total = coarse[k, 1] + DT * u
        frame[2 * PAD : 2 * PAD + half, :] = (DT * inner[k]) * total
        spread = laplacian(frame, PAD, rows) * (DT * far[k])
        v = (1.0 - (DT * DAMP) * inner[k]) * total
        middle = near[k] * total + far[k, PAD : PAD + half, :] * (v + DT * u)
        above = above + jnp.sum(spread[:PAD], axis=0, keepdims=True)
        middle = middle + spread[PAD : PAD + half]
        amid = amid + jnp.sum(middle, axis=0, keepdims=True)
        below = below + jnp.sum(spread[PAD + half :], axis=0, keepdims=True)
    gradient = jnp.zeros((1, 128), jnp.float32)
    gradient = add_tiles(gradient, tile_map, (first + TILE - 1) // TILE - 1, above)
    gradient = add_tiles(gradient, tile_map, first // TILE, amid)
    gradient = add_tiles(gradient, tile_map, (first + half) // TILE, below)
    partial[...] = gradient


def pass_kernel(place, coarse, edge, preceding, forward_edge, after, out):
    strip, core = place_of(place)
    half = coarse.shape[2]
    for i in range(2):
        out[half * i : half * i + half, :] = coarse[1 - core, i]
        out[half * (2 + i) : half * (3 + i), :] = jnp.where(core == 0, coarse[0, i], preceding[i])
        row = 4 * half + PAD * i
        out[row : row + PAD, :] = edge[at(PAD * (2 * (1 - core) + i), PAD), :]
    out[4 * half + 2 * PAD :, :] = forward_edge[4 * PAD :, :]


def adjoint_kernel(
    strips,
    place, step, modulation, tile_map, coarse, edge, preceding, forward_edge, came, eps,
    adjoint_u, adjoint_v,
    frame, field, static, before,
):
    strip, core = place_of(place)
    rows, width = eps.shape
    half = rows // 2
    count = rows + 2 * PAD
    here = at(PAD + half * core, half)
    there = at(PAD + half * (1 - core), half)
    near = at((rows + PAD) * core, PAD)
    far = at((rows + PAD) * (1 - core), PAD)
    for i in range(2):
        field[i, here, :] = coarse[core, i]
        field[i, there, :] = came[half * i : half * i + half, :]
        field[i, near, :] = edge[at(PAD * (2 * core + i), PAD), :]
        row = 4 * half + PAD * i
        field[i, far, :] = came[row : row + PAD, :]
        before[i, at(half * core, half), :] = jnp.where(core == 0, preceding[i], coarse[0, i])
        before[i, at(half * (1 - core), half), :] = came[half * (2 + i) : half * (3 + i), :]
    static[PAD : PAD + rows, :] = eps[...]
    static[near, :] = forward_edge[4 * PAD :, :]
    static[far, :] = came[4 * half + 2 * PAD :, :]

    line = lax.broadcasted_iota(jnp.int32, (count, width), 0)
    lowest = jnp.where(strip > 0, 0, PAD)
    highest = jnp.where(strip < strips - 1, count, PAD + rows)
    in_grid = jnp.logical_and(line >= lowest, line < highest)
    steady = jnp.where(in_grid, static[...], 1.0)
    depth = depth_rows(modulation, tile_map, strip * rows, rows)
    start = jnp.full((1, 1), step[0].astype(jnp.float32))
    inverse = [1.0 / (steady * (1.0 + depth * cosine(start, level))) for level in range(2)]
    inner = slice(PAD, PAD + rows)
    frame[:PAD, :] = jnp.zeros((PAD, width), jnp.float32)
    frame[PAD + count :, :] = jnp.zeros((PAD, width), jnp.float32)
    u = field[0]
    total = field[1] + DT * u
    frame[PAD : PAD + count, :] = (DT * inverse[1]) * total
    u = u + laplacian(frame, PAD, count)
    total = (1.0 - (DT * DAMP) * inverse[1]) * total + DT * u
    frame[PAD : PAD + count, :] = jnp.where(in_grid, (DT * inverse[0]) * total, 0.0)
    adjoint_u[...] = u[inner] + laplacian(frame, 2 * PAD, rows) - before[0]
    adjoint_v[...] = (1.0 - (DT * DAMP) * inverse[0][inner]) * total[inner] - before[1]


def shifted(array, axis, by):
    length = lax.axis_size(axis)
    return lax.ppermute(array, axis, [(i, (i + by) % length) for i in range(length)])


def swapped(edge):
    strips = lax.axis_size(STRIP)
    pairs = [(strips + i, i + 1) for i in range(strips - 1)]
    return lax.ppermute(edge, HALVES, pairs + [(b, a) for a, b in pairs])


def summed(array, axes):
    count = lax.axis_size(axes)
    copies = jnp.broadcast_to(array[None], (count,) + array.shape)
    pieces = lax.all_to_all(copies, axes, 0, 0, tiled=True)
    return jnp.sum(pieces, axis=0)


def shards(forward_u, forward_v, permittivity, coarse_rate, modulation, tile_map, start_step):
    rows, width = permittivity.shape
    half = rows // 2
    strips = lax.axis_size(STRIP)
    slices = lax.axis_size(TM)
    pairs = lax.axis_size(CHIPS)
    tiles = half // 8 * (width // 128)
    held = tiles // pairs
    place = (2 * lax.axis_index(STRIP) + lax.axis_index(CORE)).astype(jnp.int32).reshape(1)
    inputs = [forward_u[0], forward_v[0], coarse_rate[0]]
    tail = PAD
    state = (2, half, width)

    (send,) = call(
        gather_kernel, [SMEM, SMEM] + [HBM] * 3, [(3 * (half + PAD) + tail, width)],
        [pltpu.SemaphoreType.DMA((3,))],
    )(place, start_step, *[pltpu.with_memory_space_constraint(field, pltpu.HBM) for field in inputs])
    came = shifted(send, CORE, 1)
    fields, early, edge = call(
        sort_kernel, [SMEM] + [VMEM] * 5,
        [(2, 3, half + PAD, width), state, (5 * PAD, width)],
    )(place, *inputs, permittivity, came)
    following = shifted(early, CHIPS, -1)
    forward_edge = swapped(edge)
    maps, keep, near, far, inner = call(
        functools.partial(forward_kernel, slices, strips),
        [SMEM] * 4 + [VMEM] * 5,
        [(tiles, 24, 128), (2, 3, half, width), state, (2, half + 2 * PAD, width), state],
        [(half + 4 * PAD, width), (2, half + 2 * PAD, width), (half + 2 * PAD, width)],
    )(place, start_step, modulation, tile_map, fields, permittivity, came, forward_edge, following)

    maps = lax.all_to_all(maps.reshape(pairs, held * 24, 128), CHIPS, 0, 0, tiled=True)
    (carries,) = call(cycle_kernel, [VMEM], [(pairs, held, 16, 128)])(
        maps.reshape(pairs, held, 24, 128)
    )
    carries = lax.all_to_all(carries.reshape(pairs, held * 16, 128), CHIPS, 0, 0, tiled=True)

    coarse, late, edge, partial = call(
        spread_kernel, [SMEM, SMEM] + [VMEM] * 5,
        [(2, 2, half, width), state, (4 * PAD, width), (1, 128)],
        [(half + 4 * PAD, width)],
    )(place, tile_map, carries.reshape(tiles, 16, 128), keep, near, far, inner)
    preceding = shifted(late, CHIPS, 1)
    edge = swapped(edge)
    total = summed(partial, TM)
    (send,) = call(pass_kernel, [SMEM] + [VMEM] * 5, [(4 * half + 3 * PAD, width)])(
        place, coarse, edge, preceding, forward_edge, total
    )
    total = summed(total, STRIP)
    came = shifted(send, CORE, 1)
    adjoint_u, adjoint_v = call(
        functools.partial(adjoint_kernel, strips),
        [SMEM] * 4 + [VMEM] * 6,
        [(rows, width), (rows, width)],
        [
            (rows + 4 * PAD, width), (2, rows + 2 * PAD, width),
            (rows + 2 * PAD, width), (2, rows, width),
        ],
    )(
        place, start_step, modulation, tile_map, coarse, edge, preceding, forward_edge, came,
        permittivity,
    )
    depth_grad = total[0, : modulation.shape[0]]
    return (adjoint_u[None], adjoint_v[None], depth_grad)


def solution(mesh):
    torus = Mesh(
        mesh.devices.reshape(4, 8, 2, 2, 4), ("tm_0", "tm_1", "tm_2", "strip_0", "strip_1")
    )
    return on_torus(torus)


def on_torus(torus):
    placed = (
        P(TM, STRIP, None),
        P(TM, STRIP, None),
        P(STRIP, None),
        P(TM, STRIP, None),
        P(),
        P(),
        P(TM),
    )
    return jax.shard_map(
        shards,
        mesh=torus,
        in_specs=placed,
        out_specs=(P(TM, STRIP, None), P(TM, STRIP, None), P()),
        check_vma=False,
    )
```

```python
import functools

import jax
import jax.numpy as jnp
from jax import lax
from jax.experimental import pallas as pl
from jax.experimental.pallas import tpu as pltpu
from jax.sharding import Mesh
from jax.sharding import PartitionSpec as P

TILE = 128
PERIOD = 256
STRIP = ("strip_0", "strip_1")
TM = ("tm_0", "tm_1", "tm_2")
CHIPS = ("tm_0", "tm_1")
CORE = "tm_2"
PAD = 8

COEF = (-205.0 / 72.0, 8.0 / 5.0, -1.0 / 5.0, 8.0 / 315.0, -1.0 / 560.0)
DT = 0.4
DAMP = 0.1

INTERPRET = False
VMEM_LIMIT = 12 * 1024 * 1024

LAYER = ("tm_1", "tm_2", "strip_1")
RING = ("tm_0", "strip_0")
HALVES = (CORE,) + STRIP
VMEM = pl.BlockSpec(memory_space=pltpu.VMEM)
SMEM = pl.BlockSpec(memory_space=pltpu.SMEM)
HBM = pl.BlockSpec(memory_space=pltpu.HBM)


def held(shape):
    return pltpu.VMEM(shape, jnp.float32) if isinstance(shape, tuple) else shape


def call(kernel, ins, outs, scratch=()):
    return pl.pallas_call(
        kernel,
        in_specs=ins,
        out_specs=[VMEM] * len(outs),
        out_shape=[jax.ShapeDtypeStruct(shape, jnp.float32) for shape in outs],
        scratch_shapes=[held(shape) for shape in scratch],
        compiler_params=pltpu.CompilerParams(vmem_limit_bytes=VMEM_LIMIT),
        interpret=INTERPRET,
    )


def laplacian(frame, first, count):
    width = frame.shape[1]
    center = frame[first : first + count, :]
    summed = (2.0 * COEF[0]) * center
    for j in range(1, 5):
        rows = frame[first + j : first + j + count, :] + frame[first - j : first - j + count, :]
        cols = pltpu.roll(center, j, 1) + pltpu.roll(center, width - j, 1)
        summed = summed + COEF[j] * (rows + cols)
    return summed


def depth_row(modulation, tile_map, row, count):
    row = jnp.clip(row, 0, tile_map.shape[0] - 1)
    parts = [
        jnp.full((count, TILE), modulation[tile_map[row, j]], jnp.float32)
        for j in range(tile_map.shape[1])
    ]
    return jnp.concatenate(parts, axis=1)


def depth_rows(modulation, tile_map, first, rows):
    return jnp.concatenate(
        [
            depth_row(modulation, tile_map, (first + TILE - 1) // TILE - 1, PAD),
            depth_row(modulation, tile_map, first // TILE, rows),
            depth_row(modulation, tile_map, (first + rows) // TILE, PAD),
        ],
        axis=0,
    )


def cosine(step, level):
    offset = jnp.broadcast_to(step + float(level), (8, 128))
    return jnp.cos((2.0 * jnp.pi / PERIOD) * offset)[:1, :1]


def place_of(place):
    return place[0] // 2, place[0] % 2


def at(start, count):
    return pl.ds(pl.multiple_of(start, PAD), count)


def gather_kernel(place, step, u, v, rate, out, sems):
    strip, core = place_of(place)
    count = u.shape[0] // 2 + PAD
    rows = at((count - 2 * PAD) * (1 - core), count)
    copies = [
        pltpu.make_async_copy(field.at[rows, :], out.at[pl.ds(count * i, count), :], sems.at[i])
        for i, field in enumerate((u, v, rate))
    ]
    for copy in copies:
        copy.start()
    tail = out.shape[0] - 3 * count
    out[3 * count :, :] = jnp.full((tail, out.shape[1]), step[0].astype(jnp.float32))
    for copy in copies:
        copy.wait()


def sort_kernel(place, u, v, rate, eps, came, state, early, edge):
    strip, core = place_of(place)
    half = u.shape[0] // 2
    count = half + PAD
    rows = at((half - PAD) * core, count)
    for i, field in enumerate((u, v, rate)):
        state[core, i] = field[rows, :]
        state[1 - core, i] = came[count * i : count * i + count, :]
    for i in range(2):
        early[i] = state[0, i, at(PAD * core, half), :]
    for k in range(2):
        for i in range(2):
            row = PAD * (2 * k + i)
            edge[row : row + PAD, :] = state[k, i, at(half * core, PAD), :]
    edge[4 * PAD :, :] = eps[at((2 * half - PAD) * core, PAD), :]


def forward_kernel(
    slices, strips,
    place, step, modulation, tile_map, state, eps, came, edge,
    keep, near, far, inner,
    frame, field, static,
):
    strip, core = place_of(place)
    half = eps.shape[0] // 2
    width = eps.shape[1]
    rows = half + 2 * PAD
    first = (2 * strip + core) * half
    line = lax.broadcasted_iota(jnp.int32, (rows, width), 0)
    lowest = jnp.where(first > 0, 0, PAD)
    highest = jnp.where(first + half < strips * 2 * half, rows, half + PAD)
    in_grid = jnp.logical_and(line >= lowest, line < highest)
    body = at(PAD * (1 - core), half + PAD)
    rim = at((half + PAD) * core, PAD)

    static[body, :] = eps[at((half - PAD) * core, half + PAD), :]
    static[rim, :] = edge[4 * PAD :, :]
    steady = jnp.where(in_grid, static[...], 1.0)
    depth = depth_rows(modulation, tile_map, first, half)
    mid = slice(PAD, PAD + half)
    own = jnp.full((1, 1), step[0].astype(jnp.float32))
    other = came[came.shape[0] - 1 :, :1]
    for k in range(2):
        start = jnp.where(core == k, own, other)
        cosines = [cosine(start, level) for level in range(2)]
        inverse = [1.0 / (steady * (1.0 + depth * cosines[level])) for level in range(2)]
        for i in range(2):
            field[i, body, :] = state[k, i]
            field[i, rim, :] = edge[PAD * (2 * k + i) : PAD * (2 * k + i) + PAD, :]
        u = field[0]
        v = field[1]
        frame[:PAD, :] = jnp.zeros((PAD, width), jnp.float32)
        frame[PAD + rows :, :] = jnp.zeros((PAD, width), jnp.float32)
        frame[PAD : PAD + rows, :] = u
        force = laplacian(frame, PAD, rows) - DAMP * v
        weight = (cosines[0] * -DT) * force * (inverse[0] * inverse[0]) * steady
        far[k] = jnp.where(in_grid, weight, 0.0)
        v = v + DT * force * inverse[0]
        u = jnp.where(in_grid, u + DT * v, 0.0)
        frame[PAD : PAD + rows, :] = u
        v = v[mid]
        u = u[mid]
        force = laplacian(frame, 2 * PAD, half) - DAMP * v
        late = inverse[1][mid]
        near[k] = (cosines[1] * -DT) * force * (late * late) * steady[mid]
        inner[k] = late
        v = v + DT * force * late
        u = u + DT * v
        keep[k, 0] = jnp.exp(-state[k, 2, at(PAD * core, half), :] / slices)
        if k == 0:
            keep[0, 1] = u - state[1, 0, at(PAD * core, half), :]
            keep[0, 2] = v - state[1, 1, at(PAD * core, half), :]
        else:
            keep[1, 1] = u
            keep[1, 2] = v


def blocks(rows, width):
    return [(8 * i, 128 * j) for i in range(rows // 8) for j in range(width // 128)]


def pair_kernel(keep, following, maps):
    half, width = keep.shape[2:]
    for t, (r, c) in enumerate(blocks(half, width)):
        factor = keep[0, 0, r : r + 8, c : c + 128]
        maps[t, 0:8, :] = factor * keep[1, 0, r : r + 8, c : c + 128]
        for i in range(2):
            mismatch = keep[1, 1 + i, r : r + 8, c : c + 128] - following[i, r : r + 8, c : c + 128]
            maps[t, 8 * (1 + i) : 8 * (2 + i), :] = (
                factor * mismatch + keep[0, 1 + i, r : r + 8, c : c + 128]
            )


def cycle_kernel(maps, carries):
    pairs, held = maps.shape[:2]
    for t in range(held):
        a = maps[pairs - 1, t, 0:8, :]
        bu = maps[pairs - 1, t, 8:16, :]
        bv = maps[pairs - 1, t, 16:24, :]
        for p in reversed(range(pairs - 1)):
            factor = maps[p, t, 0:8, :]
            a = factor * a
            bu = factor * bu + maps[p, t, 8:16, :]
            bv = factor * bv + maps[p, t, 16:24, :]
        share = 1.0 / (1.0 - a)
        u = bu * share
        v = bv * share
        for p in reversed(range(pairs)):
            carries[p, t, 0:8, :] = u
            carries[p, t, 8:16, :] = v
            if p:
                factor = maps[p, t, 0:8, :]
                u = factor * u + maps[p, t, 8:16, :]
                v = factor * v + maps[p, t, 16:24, :]


def add_tiles(gradient, tile_map, row, column):
    lanes = lax.broadcasted_iota(jnp.int32, (1, 128), 1)
    row = jnp.clip(row, 0, tile_map.shape[0] - 1)
    for j in range(tile_map.shape[1]):
        amount = jnp.sum(column[:, j * TILE : (j + 1) * TILE], axis=1, keepdims=True)
        gradient = gradient + jnp.where(lanes == tile_map[row, j], amount, 0.0)
    return gradient


def spread_kernel(
    place, tile_map, carries, keep, following, near, far, inner,
    coarse, late, edge, partial, frame,
):
    strip, core = place_of(place)
    half, width = keep.shape[2:]
    rows = half + 2 * PAD
    first = (2 * strip + core) * half
    for t, (r, c) in enumerate(blocks(half, width)):
        for i in range(2):
            entering = carries[t, 8 * i : 8 * i + 8, :]
            mismatch = keep[1, 1 + i, r : r + 8, c : c + 128] - following[i, r : r + 8, c : c + 128]
            entering = keep[1, 0, r : r + 8, c : c + 128] * entering + mismatch
            coarse[1, i, r : r + 8, c : c + 128] = entering
            coarse[0, i, r : r + 8, c : c + 128] = (
                keep[0, 0, r : r + 8, c : c + 128] * entering
                + keep[0, 1 + i, r : r + 8, c : c + 128]
            )
    frame[...] = jnp.zeros_like(frame)
    above = jnp.zeros((1, width), jnp.float32)
    amid = jnp.zeros((1, width), jnp.float32)
    below = jnp.zeros((1, width), jnp.float32)
    for k in range(2):
        for i in range(2):
            late[i] = coarse[1, i]
            row = PAD * (2 * k + i)
            edge[row : row + PAD, :] = coarse[k, i, at((half - PAD) * core, PAD), :]
        u = coarse[k, 0]
        total = coarse[k, 1] + DT * u
        frame[2 * PAD : 2 * PAD + half, :] = (DT * inner[k]) * total
        spread = laplacian(frame, PAD, rows) * (DT * far[k])
        v = (1.0 - (DT * DAMP) * inner[k]) * total
        middle = near[k] * total + far[k, PAD : PAD + half, :] * (v + DT * u)
        above = above + jnp.sum(spread[:PAD], axis=0, keepdims=True)
        middle = middle + spread[PAD : PAD + half]
        amid = amid + jnp.sum(middle, axis=0, keepdims=True)
        below = below + jnp.sum(spread[PAD + half :], axis=0, keepdims=True)
    gradient = jnp.zeros((1, 128), jnp.float32)
    gradient = add_tiles(gradient, tile_map, (first + TILE - 1) // TILE - 1, above)
    gradient = add_tiles(gradient, tile_map, first // TILE, amid)
    gradient = add_tiles(gradient, tile_map, (first + half) // TILE, below)
    partial[...] = gradient


def pass_kernel(place, coarse, edge, preceding, forward_edge, after, out):
    strip, core = place_of(place)
    half = coarse.shape[2]
    for i in range(2):
        out[half * i : half * i + half, :] = coarse[1 - core, i]
        out[half * (2 + i) : half * (3 + i), :] = jnp.where(core == 0, coarse[0, i], preceding[i])
        row = 4 * half + PAD * i
        out[row : row + PAD, :] = edge[at(PAD * (2 * (1 - core) + i), PAD), :]
    out[4 * half + 2 * PAD :, :] = forward_edge[4 * PAD :, :]


def adjoint_kernel(
    strips,
    place, step, modulation, tile_map, coarse, edge, preceding, forward_edge, came, eps,
    adjoint_u, adjoint_v,
    frame, field, static, before,
):
    strip, core = place_of(place)
    rows, width = eps.shape
    half = rows // 2
    count = rows + 2 * PAD
    here = at(PAD + half * core, half)
    there = at(PAD + half * (1 - core), half)
    near = at((rows + PAD) * core, PAD)
    far = at((rows + PAD) * (1 - core), PAD)
    for i in range(2):
        field[i, here, :] = coarse[core, i]
        field[i, there, :] = came[half * i : half * i + half, :]
        field[i, near, :] = edge[at(PAD * (2 * core + i), PAD), :]
        row = 4 * half + PAD * i
        field[i, far, :] = came[row : row + PAD, :]
        before[i, at(half * core, half), :] = jnp.where(core == 0, preceding[i], coarse[0, i])
        before[i, at(half * (1 - core), half), :] = came[half * (2 + i) : half * (3 + i), :]
    static[PAD : PAD + rows, :] = eps[...]
    static[near, :] = forward_edge[4 * PAD :, :]
    static[far, :] = came[4 * half + 2 * PAD :, :]

    line = lax.broadcasted_iota(jnp.int32, (count, width), 0)
    lowest = jnp.where(strip > 0, 0, PAD)
    highest = jnp.where(strip < strips - 1, count, PAD + rows)
    in_grid = jnp.logical_and(line >= lowest, line < highest)
    steady = jnp.where(in_grid, static[...], 1.0)
    depth = depth_rows(modulation, tile_map, strip * rows, rows)
    start = jnp.full((1, 1), step[0].astype(jnp.float32))
    inverse = [1.0 / (steady * (1.0 + depth * cosine(start, level))) for level in range(2)]
    inner = slice(PAD, PAD + rows)
    frame[:PAD, :] = jnp.zeros((PAD, width), jnp.float32)
    frame[PAD + count :, :] = jnp.zeros((PAD, width), jnp.float32)
    u = field[0]
    total = field[1] + DT * u
    frame[PAD : PAD + count, :] = (DT * inverse[1]) * total
    u = u + laplacian(frame, PAD, count)
    total = (1.0 - (DT * DAMP) * inverse[1]) * total + DT * u
    frame[PAD : PAD + count, :] = jnp.where(in_grid, (DT * inverse[0]) * total, 0.0)
    adjoint_u[...] = u[inner] + laplacian(frame, 2 * PAD, rows) - before[0]
    adjoint_v[...] = (1.0 - (DT * DAMP) * inverse[0][inner]) * total[inner] - before[1]


def shifted(array, axis, by):
    length = lax.axis_size(axis)
    return lax.ppermute(array, axis, [(i, (i + by) % length) for i in range(length)])


def swapped(edge):
    strips = lax.axis_size(STRIP)
    pairs = [(strips + i, i + 1) for i in range(strips - 1)]
    return lax.ppermute(edge, HALVES, pairs + [(b, a) for a, b in pairs])


def summed(array, axes):
    count = lax.axis_size(axes)
    copies = jnp.broadcast_to(array[None], (count,) + array.shape)
    pieces = lax.all_to_all(copies, axes, 0, 0, tiled=True)
    return jnp.sum(pieces, axis=0)


def shards(forward_u, forward_v, permittivity, coarse_rate, modulation, tile_map, start_step):
    rows, width = permittivity.shape
    half = rows // 2
    strips = lax.axis_size(STRIP)
    slices = lax.axis_size(TM)
    pairs = lax.axis_size(CHIPS)
    tiles = half // 8 * (width // 128)
    held = tiles // pairs
    place = (2 * lax.axis_index(STRIP) + lax.axis_index(CORE)).astype(jnp.int32).reshape(1)
    inputs = [forward_u[0], forward_v[0], coarse_rate[0]]
    tail = PAD
    state = (2, half, width)

    (send,) = call(
        gather_kernel, [SMEM, SMEM] + [HBM] * 3, [(3 * (half + PAD) + tail, width)],
        [pltpu.SemaphoreType.DMA((3,))],
    )(place, start_step, *[pltpu.with_memory_space_constraint(field, pltpu.HBM) for field in inputs])
    came = shifted(send, CORE, 1)
    fields, early, edge = call(
        sort_kernel, [SMEM] + [VMEM] * 5,
        [(2, 3, half + PAD, width), state, (5 * PAD, width)],
    )(place, *inputs, permittivity, came)
    following = shifted(early, CHIPS, -1)
    forward_edge = swapped(edge)
    keep, near, far, inner = call(
        functools.partial(forward_kernel, slices, strips),
        [SMEM] * 4 + [VMEM] * 4,
        [(2, 3, half, width), state, (2, half + 2 * PAD, width), state],
        [(half + 4 * PAD, width), (2, half + 2 * PAD, width), (half + 2 * PAD, width)],
    )(place, start_step, modulation, tile_map, fields, permittivity, came, forward_edge)
    (maps,) = call(pair_kernel, [VMEM] * 2, [(tiles, 24, 128)])(keep, following)

    maps = lax.all_to_all(maps.reshape(pairs, held * 24, 128), CHIPS, 0, 0, tiled=True)
    (carries,) = call(cycle_kernel, [VMEM], [(pairs, held, 16, 128)])(
        maps.reshape(pairs, held, 24, 128)
    )
    carries = lax.all_to_all(carries.reshape(pairs, held * 16, 128), CHIPS, 0, 0, tiled=True)

    coarse, late, edge, partial = call(
        spread_kernel, [SMEM, SMEM] + [VMEM] * 6,
        [(2, 2, half, width), state, (4 * PAD, width), (1, 128)],
        [(half + 4 * PAD, width)],
    )(place, tile_map, carries.reshape(tiles, 16, 128), keep, following, near, far, inner)
    preceding = shifted(late, CHIPS, 1)
    edge = swapped(edge)
    total = summed(partial, LAYER)
    (send,) = call(pass_kernel, [SMEM] + [VMEM] * 5, [(4 * half + 3 * PAD, width)])(
        place, coarse, edge, preceding, forward_edge, total
    )
    total = summed(total, RING)
    came = shifted(send, CORE, 1)
    adjoint_u, adjoint_v = call(
        functools.partial(adjoint_kernel, strips),
        [SMEM] * 4 + [VMEM] * 6,
        [(rows, width), (rows, width)],
        [
            (rows + 4 * PAD, width), (2, rows + 2 * PAD, width),
            (rows + 2 * PAD, width), (2, rows, width),
        ],
    )(
        place, start_step, modulation, tile_map, coarse, edge, preceding, forward_edge, came,
        permittivity,
    )
    depth_grad = total[0, : modulation.shape[0]]
    return (adjoint_u[None], adjoint_v[None], depth_grad)


def solution(mesh):
    torus = Mesh(
        mesh.devices.reshape(4, 8, 2, 2, 4), ("tm_0", "tm_1", "tm_2", "strip_0", "strip_1")
    )
    return on_torus(torus)


def on_torus(torus):
    placed = (
        P(TM, STRIP, None),
        P(TM, STRIP, None),
        P(STRIP, None),
        P(TM, STRIP, None),
        P(),
        P(),
        P(TM),
    )
    return jax.shard_map(
        shards,
        mesh=torus,
        in_specs=placed,
        out_specs=(P(TM, STRIP, None), P(TM, STRIP, None), P()),
        check_vma=False,
    )
```

```python
import functools

import jax
import jax.numpy as jnp
from jax import lax
from jax.experimental import pallas as pl
from jax.experimental.pallas import tpu as pltpu
from jax.sharding import Mesh
from jax.sharding import PartitionSpec as P

TILE = 128
PERIOD = 256
STRIP = ("strip_0", "strip_1")
TM = ("tm_0", "tm_1", "tm_2")
CHIPS = ("tm_0", "tm_1")
CORE = "tm_2"
PAD = 8

COEF = (-205.0 / 72.0, 8.0 / 5.0, -1.0 / 5.0, 8.0 / 315.0, -1.0 / 560.0)
DT = 0.4
DAMP = 0.1

INTERPRET = False
VMEM_LIMIT = 12 * 1024 * 1024

ALL_CHIPS = ("tm_0", "tm_1", "strip_0", "strip_1")
HALVES = (CORE,) + STRIP
VMEM = pl.BlockSpec(memory_space=pltpu.VMEM)
SMEM = pl.BlockSpec(memory_space=pltpu.SMEM)
HBM = pl.BlockSpec(memory_space=pltpu.HBM)


def held(shape):
    return pltpu.VMEM(shape, jnp.float32) if isinstance(shape, tuple) else shape


def call(kernel, ins, outs, scratch=()):
    return pl.pallas_call(
        kernel,
        in_specs=ins,
        out_specs=[VMEM] * len(outs),
        out_shape=[jax.ShapeDtypeStruct(shape, jnp.float32) for shape in outs],
        scratch_shapes=[held(shape) for shape in scratch],
        compiler_params=pltpu.CompilerParams(vmem_limit_bytes=VMEM_LIMIT),
        interpret=INTERPRET,
    )


def laplacian(frame, first, count):
    width = frame.shape[1]
    center = frame[first : first + count, :]
    summed = (2.0 * COEF[0]) * center
    for j in range(1, 5):
        rows = frame[first + j : first + j + count, :] + frame[first - j : first - j + count, :]
        cols = pltpu.roll(center, j, 1) + pltpu.roll(center, width - j, 1)
        summed = summed + COEF[j] * (rows + cols)
    return summed


def depth_row(modulation, tile_map, row, count):
    row = jnp.clip(row, 0, tile_map.shape[0] - 1)
    parts = [
        jnp.full((count, TILE), modulation[tile_map[row, j]], jnp.float32)
        for j in range(tile_map.shape[1])
    ]
    return jnp.concatenate(parts, axis=1)


def depth_rows(modulation, tile_map, first, rows):
    return jnp.concatenate(
        [
            depth_row(modulation, tile_map, (first + TILE - 1) // TILE - 1, PAD),
            depth_row(modulation, tile_map, first // TILE, rows),
            depth_row(modulation, tile_map, (first + rows) // TILE, PAD),
        ],
        axis=0,
    )


def cosine(step, level):
    offset = jnp.broadcast_to(step + float(level), (8, 128))
    return jnp.cos((2.0 * jnp.pi / PERIOD) * offset)[:1, :1]


def place_of(place):
    return place[0] // 2, place[0] % 2


def at(start, count):
    return pl.ds(pl.multiple_of(start, PAD), count)


def gather_kernel(place, step, u, v, rate, out, sems):
    strip, core = place_of(place)
    count = u.shape[0] // 2 + PAD
    rows = at((count - 2 * PAD) * (1 - core), count)
    copies = [
        pltpu.make_async_copy(field.at[rows, :], out.at[pl.ds(count * i, count), :], sems.at[i])
        for i, field in enumerate((u, v, rate))
    ]
    for copy in copies:
        copy.start()
    tail = out.shape[0] - 3 * count
    out[3 * count :, :] = jnp.full((tail, out.shape[1]), step[0].astype(jnp.float32))
    for copy in copies:
        copy.wait()


def sort_kernel(place, u, v, rate, eps, came, state, early, edge):
    strip, core = place_of(place)
    half = u.shape[0] // 2
    count = half + PAD
    rows = at((half - PAD) * core, count)
    for i, field in enumerate((u, v, rate)):
        state[core, i] = field[rows, :]
        state[1 - core, i] = came[count * i : count * i + count, :]
    for i in range(2):
        early[i] = state[0, i, at(PAD * core, half), :]
    for k in range(2):
        for i in range(2):
            row = PAD * (2 * k + i)
            edge[row : row + PAD, :] = state[k, i, at(half * core, PAD), :]
    edge[4 * PAD :, :] = eps[at((2 * half - PAD) * core, PAD), :]


def forward_kernel(
    slices, strips,
    place, step, modulation, tile_map, state, eps, came, edge,
    keep, near, far, inner,
    frame, field, static,
):
    strip, core = place_of(place)
    half = eps.shape[0] // 2
    width = eps.shape[1]
    rows = half + 2 * PAD
    first = (2 * strip + core) * half
    line = lax.broadcasted_iota(jnp.int32, (rows, width), 0)
    lowest = jnp.where(first > 0, 0, PAD)
    highest = jnp.where(first + half < strips * 2 * half, rows, half + PAD)
    in_grid = jnp.logical_and(line >= lowest, line < highest)
    body = at(PAD * (1 - core), half + PAD)
    rim = at((half + PAD) * core, PAD)

    static[body, :] = eps[at((half - PAD) * core, half + PAD), :]
    static[rim, :] = edge[4 * PAD :, :]
    steady = jnp.where(in_grid, static[...], 1.0)
    depth = depth_rows(modulation, tile_map, first, half)
    mid = slice(PAD, PAD + half)
    own = jnp.full((1, 1), step[0].astype(jnp.float32))
    other = came[came.shape[0] - 1 :, :1]
    for k in range(2):
        start = jnp.where(core == k, own, other)
        cosines = [cosine(start, level) for level in range(2)]
        inverse = [1.0 / (steady * (1.0 + depth * cosines[level])) for level in range(2)]
        for i in range(2):
            field[i, body, :] = state[k, i]
            field[i, rim, :] = edge[PAD * (2 * k + i) : PAD * (2 * k + i) + PAD, :]
        u = field[0]
        v = field[1]
        frame[:PAD, :] = jnp.zeros((PAD, width), jnp.float32)
        frame[PAD + rows :, :] = jnp.zeros((PAD, width), jnp.float32)
        frame[PAD : PAD + rows, :] = u
        force = laplacian(frame, PAD, rows) - DAMP * v
        weight = (cosines[0] * -DT) * force * (inverse[0] * inverse[0]) * steady
        far[k] = jnp.where(in_grid, weight, 0.0)
        v = v + DT * force * inverse[0]
        u = jnp.where(in_grid, u + DT * v, 0.0)
        frame[PAD : PAD + rows, :] = u
        v = v[mid]
        u = u[mid]
        force = laplacian(frame, 2 * PAD, half) - DAMP * v
        late = inverse[1][mid]
        near[k] = (cosines[1] * -DT) * force * (late * late) * steady[mid]
        inner[k] = late
        v = v + DT * force * late
        u = u + DT * v
        keep[k, 0] = jnp.exp(-state[k, 2, at(PAD * core, half), :] / slices)
        if k == 0:
            keep[0, 1] = u - state[1, 0, at(PAD * core, half), :]
            keep[0, 2] = v - state[1, 1, at(PAD * core, half), :]
        else:
            keep[1, 1] = u
            keep[1, 2] = v


def blocks(rows, width):
    return [(8 * i, 128 * j) for i in range(rows // 8) for j in range(width // 128)]


def pair_kernel(keep, following, maps):
    half, width = keep.shape[2:]
    for t, (r, c) in enumerate(blocks(half, width)):
        factor = keep[0, 0, r : r + 8, c : c + 128]
        maps[t, 0:8, :] = factor * keep[1, 0, r : r + 8, c : c + 128]
        for i in range(2):
            mismatch = keep[1, 1 + i, r : r + 8, c : c + 128] - following[i, r : r + 8, c : c + 128]
            maps[t, 8 * (1 + i) : 8 * (2 + i), :] = (
                factor * mismatch + keep[0, 1 + i, r : r + 8, c : c + 128]
            )


def cycle_kernel(maps, carries):
    pairs, held = maps.shape[:2]
    for t in range(held):
        a = maps[pairs - 1, t, 0:8, :]
        bu = maps[pairs - 1, t, 8:16, :]
        bv = maps[pairs - 1, t, 16:24, :]
        for p in reversed(range(pairs - 1)):
            factor = maps[p, t, 0:8, :]
            a = factor * a
            bu = factor * bu + maps[p, t, 8:16, :]
            bv = factor * bv + maps[p, t, 16:24, :]
        share = 1.0 / (1.0 - a)
        u = bu * share
        v = bv * share
        for p in reversed(range(pairs)):
            carries[p, t, 0:8, :] = u
            carries[p, t, 8:16, :] = v
            if p:
                factor = maps[p, t, 0:8, :]
                u = factor * u + maps[p, t, 8:16, :]
                v = factor * v + maps[p, t, 16:24, :]


def add_tiles(gradient, tile_map, row, column):
    lanes = lax.broadcasted_iota(jnp.int32, (1, 128), 1)
    row = jnp.clip(row, 0, tile_map.shape[0] - 1)
    for j in range(tile_map.shape[1]):
        amount = jnp.sum(column[:, j * TILE : (j + 1) * TILE], axis=1, keepdims=True)
        gradient = gradient + jnp.where(lanes == tile_map[row, j], amount, 0.0)
    return gradient


def spread_kernel(
    place, tile_map, carries, keep, following, near, far, inner,
    coarse, late, edge, partial, frame,
):
    strip, core = place_of(place)
    half, width = keep.shape[2:]
    rows = half + 2 * PAD
    first = (2 * strip + core) * half
    for t, (r, c) in enumerate(blocks(half, width)):
        for i in range(2):
            entering = carries[t, 8 * i : 8 * i + 8, :]
            mismatch = keep[1, 1 + i, r : r + 8, c : c + 128] - following[i, r : r + 8, c : c + 128]
            entering = keep[1, 0, r : r + 8, c : c + 128] * entering + mismatch
            coarse[1, i, r : r + 8, c : c + 128] = entering
            coarse[0, i, r : r + 8, c : c + 128] = (
                keep[0, 0, r : r + 8, c : c + 128] * entering
                + keep[0, 1 + i, r : r + 8, c : c + 128]
            )
    frame[...] = jnp.zeros_like(frame)
    above = jnp.zeros((1, width), jnp.float32)
    amid = jnp.zeros((1, width), jnp.float32)
    below = jnp.zeros((1, width), jnp.float32)
    for k in range(2):
        for i in range(2):
            late[i] = coarse[1, i]
            row = PAD * (2 * k + i)
            edge[row : row + PAD, :] = coarse[k, i, at((half - PAD) * core, PAD), :]
        u = coarse[k, 0]
        total = coarse[k, 1] + DT * u
        frame[2 * PAD : 2 * PAD + half, :] = (DT * inner[k]) * total
        spread = laplacian(frame, PAD, rows) * (DT * far[k])
        v = (1.0 - (DT * DAMP) * inner[k]) * total
        middle = near[k] * total + far[k, PAD : PAD + half, :] * (v + DT * u)
        above = above + jnp.sum(spread[:PAD], axis=0, keepdims=True)
        middle = middle + spread[PAD : PAD + half]
        amid = amid + jnp.sum(middle, axis=0, keepdims=True)
        below = below + jnp.sum(spread[PAD + half :], axis=0, keepdims=True)
    gradient = jnp.zeros((1, 128), jnp.float32)
    gradient = add_tiles(gradient, tile_map, (first + TILE - 1) // TILE - 1, above)
    gradient = add_tiles(gradient, tile_map, first // TILE, amid)
    gradient = add_tiles(gradient, tile_map, (first + half) // TILE, below)
    partial[...] = gradient


def pass_kernel(place, coarse, edge, preceding, forward_edge, share, out):
    strip, core = place_of(place)
    half = coarse.shape[2]
    for i in range(2):
        out[half * i : half * i + half, :] = coarse[1 - core, i]
        out[half * (2 + i) : half * (3 + i), :] = jnp.where(core == 0, coarse[0, i], preceding[i])
        row = 4 * half + PAD * i
        out[row : row + PAD, :] = edge[at(PAD * (2 * (1 - core) + i), PAD), :]
    out[4 * half + 2 * PAD : 4 * half + 3 * PAD, :] = forward_edge[4 * PAD :, :]
    out[4 * half + 3 * PAD :, :128] = jnp.broadcast_to(share[...], (PAD, 128))


def adjoint_kernel(
    strips,
    place, step, modulation, tile_map, coarse, edge, preceding, forward_edge, came, eps, share,
    adjoint_u, adjoint_v, gradient,
    frame, field, static, before,
):
    strip, core = place_of(place)
    rows, width = eps.shape
    half = rows // 2
    count = rows + 2 * PAD
    here = at(PAD + half * core, half)
    there = at(PAD + half * (1 - core), half)
    near = at((rows + PAD) * core, PAD)
    far = at((rows + PAD) * (1 - core), PAD)
    for i in range(2):
        field[i, here, :] = coarse[core, i]
        field[i, there, :] = came[half * i : half * i + half, :]
        field[i, near, :] = edge[at(PAD * (2 * core + i), PAD), :]
        row = 4 * half + PAD * i
        field[i, far, :] = came[row : row + PAD, :]
        before[i, at(half * core, half), :] = jnp.where(core == 0, preceding[i], coarse[0, i])
        before[i, at(half * (1 - core), half), :] = came[half * (2 + i) : half * (3 + i), :]
    static[PAD : PAD + rows, :] = eps[...]
    static[near, :] = forward_edge[4 * PAD :, :]
    static[far, :] = came[4 * half + 2 * PAD : 4 * half + 3 * PAD, :]
    gradient[...] = share[...] + came[4 * half + 3 * PAD : 4 * half + 3 * PAD + 1, :128]

    line = lax.broadcasted_iota(jnp.int32, (count, width), 0)
    lowest = jnp.where(strip > 0, 0, PAD)
    highest = jnp.where(strip < strips - 1, count, PAD + rows)
    in_grid = jnp.logical_and(line >= lowest, line < highest)
    steady = jnp.where(in_grid, static[...], 1.0)
    depth = depth_rows(modulation, tile_map, strip * rows, rows)
    start = jnp.full((1, 1), step[0].astype(jnp.float32))
    inverse = [1.0 / (steady * (1.0 + depth * cosine(start, level))) for level in range(2)]
    inner = slice(PAD, PAD + rows)
    frame[:PAD, :] = jnp.zeros((PAD, width), jnp.float32)
    frame[PAD + count :, :] = jnp.zeros((PAD, width), jnp.float32)
    u = field[0]
    total = field[1] + DT * u
    frame[PAD : PAD + count, :] = (DT * inverse[1]) * total
    u = u + laplacian(frame, PAD, count)
    total = (1.0 - (DT * DAMP) * inverse[1]) * total + DT * u
    frame[PAD : PAD + count, :] = jnp.where(in_grid, (DT * inverse[0]) * total, 0.0)
    adjoint_u[...] = u[inner] + laplacian(frame, 2 * PAD, rows) - before[0]
    adjoint_v[...] = (1.0 - (DT * DAMP) * inverse[0][inner]) * total[inner] - before[1]


def shifted(array, axis, by):
    length = lax.axis_size(axis)
    return lax.ppermute(array, axis, [(i, (i + by) % length) for i in range(length)])


def swapped(edge):
    strips = lax.axis_size(STRIP)
    pairs = [(strips + i, i + 1) for i in range(strips - 1)]
    return lax.ppermute(edge, HALVES, pairs + [(b, a) for a, b in pairs])


def summed(array, axes):
    count = lax.axis_size(axes)
    copies = jnp.broadcast_to(array[None], (count,) + array.shape)
    pieces = lax.all_to_all(copies, axes, 0, 0, tiled=True)
    return jnp.sum(pieces, axis=0)


def shards(forward_u, forward_v, permittivity, coarse_rate, modulation, tile_map, start_step):
    rows, width = permittivity.shape
    half = rows // 2
    strips = lax.axis_size(STRIP)
    slices = lax.axis_size(TM)
    pairs = lax.axis_size(CHIPS)
    tiles = half // 8 * (width // 128)
    held = tiles // pairs
    place = (2 * lax.axis_index(STRIP) + lax.axis_index(CORE)).astype(jnp.int32).reshape(1)
    inputs = [forward_u[0], forward_v[0], coarse_rate[0]]
    tail = PAD
    state = (2, half, width)

    (send,) = call(
        gather_kernel, [SMEM, SMEM] + [HBM] * 3, [(3 * (half + PAD) + tail, width)],
        [pltpu.SemaphoreType.DMA((3,))],
    )(place, start_step, *[pltpu.with_memory_space_constraint(field, pltpu.HBM) for field in inputs])
    came = shifted(send, CORE, 1)
    fields, early, edge = call(
        sort_kernel, [SMEM] + [VMEM] * 5,
        [(2, 3, half + PAD, width), state, (5 * PAD, width)],
    )(place, *inputs, permittivity, came)
    following = shifted(early, CHIPS, -1)
    forward_edge = swapped(edge)
    keep, near, far, inner = call(
        functools.partial(forward_kernel, slices, strips),
        [SMEM] * 4 + [VMEM] * 4,
        [(2, 3, half, width), state, (2, half + 2 * PAD, width), state],
        [(half + 4 * PAD, width), (2, half + 2 * PAD, width), (half + 2 * PAD, width)],
    )(place, start_step, modulation, tile_map, fields, permittivity, came, forward_edge)
    (maps,) = call(pair_kernel, [VMEM] * 2, [(tiles, 24, 128)])(keep, following)

    maps = lax.all_to_all(maps.reshape(pairs, held * 24, 128), CHIPS, 0, 0, tiled=True)
    (carries,) = call(cycle_kernel, [VMEM], [(pairs, held, 16, 128)])(
        maps.reshape(pairs, held, 24, 128)
    )
    carries = lax.all_to_all(carries.reshape(pairs, held * 16, 128), CHIPS, 0, 0, tiled=True)

    coarse, late, edge, partial = call(
        spread_kernel, [SMEM, SMEM] + [VMEM] * 6,
        [(2, 2, half, width), state, (4 * PAD, width), (1, 128)],
        [(half + 4 * PAD, width)],
    )(place, tile_map, carries.reshape(tiles, 16, 128), keep, following, near, far, inner)
    preceding = shifted(late, CHIPS, 1)
    edge = swapped(edge)
    total = summed(partial, ALL_CHIPS)
    (send,) = call(pass_kernel, [SMEM] + [VMEM] * 5, [(4 * half + 4 * PAD, width)])(
        place, coarse, edge, preceding, forward_edge, total
    )
    came = shifted(send, CORE, 1)
    adjoint_u, adjoint_v, total = call(
        functools.partial(adjoint_kernel, strips),
        [SMEM] * 4 + [VMEM] * 7,
        [(rows, width), (rows, width), (1, 128)],
        [
            (rows + 4 * PAD, width), (2, rows + 2 * PAD, width),
            (rows + 2 * PAD, width), (2, rows, width),
        ],
    )(
        place, start_step, modulation, tile_map, coarse, edge, preceding, forward_edge, came,
        permittivity, total,
    )
    depth_grad = total[0, : modulation.shape[0]]
    return (adjoint_u[None], adjoint_v[None], depth_grad)


def solution(mesh):
    torus = Mesh(
        mesh.devices.reshape(4, 8, 2, 2, 4), ("tm_0", "tm_1", "tm_2", "strip_0", "strip_1")
    )
    return on_torus(torus)


def on_torus(torus):
    placed = (
        P(TM, STRIP, None),
        P(TM, STRIP, None),
        P(STRIP, None),
        P(TM, STRIP, None),
        P(),
        P(),
        P(TM),
    )
    return jax.shard_map(
        shards,
        mesh=torus,
        in_specs=placed,
        out_specs=(P(TM, STRIP, None), P(TM, STRIP, None), P()),
        check_vma=False,
    )
```

```python
import functools

import jax
import jax.numpy as jnp
from jax import lax
from jax.experimental import pallas as pl
from jax.experimental.pallas import tpu as pltpu
from jax.sharding import Mesh
from jax.sharding import PartitionSpec as P

TILE = 128
PERIOD = 256
STRIP = ("strip_0", "strip_1")
TM = ("tm_0", "tm_1", "tm_2")
CHIPS = ("tm_0", "tm_1")
CORE = "tm_2"
PAD = 8

COEF = (-205.0 / 72.0, 8.0 / 5.0, -1.0 / 5.0, 8.0 / 315.0, -1.0 / 560.0)
DT = 0.4
DAMP = 0.1

INTERPRET = False
VMEM_LIMIT = 12 * 1024 * 1024

ALL_CHIPS = ("tm_0", "tm_1", "strip_0", "strip_1")
HALVES = (CORE,) + STRIP
VMEM = pl.BlockSpec(memory_space=pltpu.VMEM)
SMEM = pl.BlockSpec(memory_space=pltpu.SMEM)
HBM = pl.BlockSpec(memory_space=pltpu.HBM)


def held(shape):
    return pltpu.VMEM(shape, jnp.float32) if isinstance(shape, tuple) else shape


def call(kernel, ins, outs, scratch=()):
    return pl.pallas_call(
        kernel,
        in_specs=ins,
        out_specs=[VMEM] * len(outs),
        out_shape=[jax.ShapeDtypeStruct(shape, jnp.float32) for shape in outs],
        scratch_shapes=[held(shape) for shape in scratch],
        compiler_params=pltpu.CompilerParams(vmem_limit_bytes=VMEM_LIMIT),
        interpret=INTERPRET,
    )


def laplacian(frame, first):
    width = frame.shape[1]
    center = frame[first : first + 8, :]
    summed = (2.0 * COEF[0]) * center
    for j in range(1, 5):
        rows = frame[first + j : first + j + 8, :] + frame[first - j : first - j + 8, :]
        cols = pltpu.roll(center, j, 1) + pltpu.roll(center, width - j, 1)
        summed = summed + COEF[j] * (rows + cols)
    return summed


def depth_row(modulation, tile_map, row, count):
    row = jnp.clip(row, 0, tile_map.shape[0] - 1)
    parts = [
        jnp.full((count, TILE), modulation[tile_map[row, j]], jnp.float32)
        for j in range(tile_map.shape[1])
    ]
    return jnp.concatenate(parts, axis=1)


def depth_blocks(modulation, tile_map, first, rows):
    above = depth_row(modulation, tile_map, (first + TILE - 1) // TILE - 1, PAD)
    amid = depth_row(modulation, tile_map, first // TILE, PAD)
    below = depth_row(modulation, tile_map, (first + rows) // TILE, PAD)
    return [above] + [amid] * (rows // 8) + [below]


def cosine(step, level):
    offset = jnp.broadcast_to(step + float(level), (8, 128))
    return jnp.cos((2.0 * jnp.pi / PERIOD) * offset)[:1, :1]


def place_of(place):
    return place[0] // 2, place[0] % 2


def at(start, count):
    return pl.ds(pl.multiple_of(start, PAD), count)


def gather_kernel(place, step, u, v, rate, out, sems):
    strip, core = place_of(place)
    count = u.shape[0] // 2 + PAD
    rows = at((count - 2 * PAD) * (1 - core), count)
    copies = [
        pltpu.make_async_copy(field.at[rows, :], out.at[pl.ds(count * i, count), :], sems.at[i])
        for i, field in enumerate((u, v, rate))
    ]
    for copy in copies:
        copy.start()
    tail = out.shape[0] - 3 * count
    out[3 * count :, :] = jnp.full((tail, out.shape[1]), step[0].astype(jnp.float32))
    for copy in copies:
        copy.wait()


def sort_kernel(place, u, v, rate, eps, came, state, early, edge):
    strip, core = place_of(place)
    half = u.shape[0] // 2
    count = half + PAD
    rows = at((half - PAD) * core, count)
    for i, field in enumerate((u, v, rate)):
        state[core, i] = field[rows, :]
        state[1 - core, i] = came[count * i : count * i + count, :]
    for i in range(2):
        early[i] = state[0, i, at(PAD * core, half), :]
    for k in range(2):
        for i in range(2):
            row = PAD * (2 * k + i)
            edge[row : row + PAD, :] = state[k, i, at(half * core, PAD), :]
    edge[4 * PAD :, :] = eps[at((2 * half - PAD) * core, PAD), :]


def forward_kernel(
    slices, strips,
    place, step, modulation, tile_map, state, eps, came, edge,
    keep, near, far, inner,
    frame, speed, static,
):
    strip, core = place_of(place)
    half = eps.shape[0] // 2
    width = eps.shape[1]
    rows = half + 2 * PAD
    first = (2 * strip + core) * half
    inside = [first > 0] + [None] * (half // 8) + [first + half < strips * 2 * half]
    body = at(PAD * (1 - core), half + PAD)
    rim = at((half + PAD) * core, PAD)

    static[body, :] = eps[at((half - PAD) * core, half + PAD), :]
    static[rim, :] = edge[4 * PAD :, :]
    for b in (0, rows // 8 - 1):
        static[8 * b : 8 * b + 8, :] = jnp.where(inside[b], static[8 * b : 8 * b + 8, :], 1.0)
    depth = depth_blocks(modulation, tile_map, first, half)
    own = jnp.full((1, 1), step[0].astype(jnp.float32))
    other = came[3 * (half + PAD) : 3 * (half + PAD) + 1, :1]
    for i in range(2):
        frame[i, :PAD, :] = jnp.zeros((PAD, width), jnp.float32)
        frame[i, PAD + rows :, :] = jnp.zeros((PAD, width), jnp.float32)
    for k in range(2):
        start = jnp.where(core == k, own, other)
        cosines = [cosine(start, level) for level in range(2)]
        frame[0, at(PAD + PAD * (1 - core), half + PAD), :] = state[k, 0]
        frame[0, at(PAD + (half + PAD) * core, PAD), :] = edge[2 * PAD * k : 2 * PAD * k + PAD, :]
        speed[body, :] = state[k, 1]
        speed[rim, :] = edge[2 * PAD * k + PAD : 2 * PAD * k + 2 * PAD, :]
        for b in range(rows // 8):
            here = slice(8 * b, 8 * b + 8)
            there = slice(PAD + 8 * b, PAD + 8 * b + 8)
            steady = static[here, :]
            inverse = 1.0 / (steady * (1.0 + depth[b] * cosines[0]))
            v = speed[here, :]
            force = laplacian(frame.at[0], PAD + 8 * b) - DAMP * v
            pull = force * inverse
            weight = (cosines[0] * -DT) * pull * inverse * steady
            v = v + DT * pull
            u = frame[0, there, :] + DT * v
            if inside[b] is not None:
                weight = jnp.where(inside[b], weight, 0.0)
                u = jnp.where(inside[b], u, 0.0)
            else:
                speed[here, :] = v
            far[k, here, :] = weight
            frame[1, there, :] = u
        for b in range(half // 8):
            here = slice(8 * b, 8 * b + 8)
            outer = slice(PAD + 8 * b, PAD + 8 * b + 8)
            steady = static[outer, :]
            inverse = 1.0 / (steady * (1.0 + depth[1 + b] * cosines[1]))
            v = speed[outer, :]
            force = laplacian(frame.at[1], 2 * PAD + 8 * b) - DAMP * v
            pull = force * inverse
            near[k, here, :] = (cosines[1] * -DT) * pull * inverse * steady
            inner[k, here, :] = inverse
            v = v + DT * pull
            u = frame[1, 2 * PAD + 8 * b : 2 * PAD + 8 * b + 8, :] + DT * v
            rows_here = at(PAD * core + 8 * b, 8)
            keep[k, 0, here, :] = jnp.exp(-state[k, 2, rows_here, :] / slices)
            if k == 0:
                u = u - state[1, 0, rows_here, :]
                v = v - state[1, 1, rows_here, :]
            keep[k, 1, here, :] = u
            keep[k, 2, here, :] = v


def blocks(rows, width):
    return [(8 * i, 128 * j) for i in range(rows // 8) for j in range(width // 128)]


def pair_kernel(keep, following, maps):
    half, width = keep.shape[2:]
    for t, (r, c) in enumerate(blocks(half, width)):
        factor = keep[0, 0, r : r + 8, c : c + 128]
        maps[t, 0:8, :] = factor * keep[1, 0, r : r + 8, c : c + 128]
        for i in range(2):
            mismatch = keep[1, 1 + i, r : r + 8, c : c + 128] - following[i, r : r + 8, c : c + 128]
            maps[t, 8 * (1 + i) : 8 * (2 + i), :] = (
                factor * mismatch + keep[0, 1 + i, r : r + 8, c : c + 128]
            )


def cycle_kernel(maps, carries):
    pairs, held = maps.shape[:2]
    for t in range(held):
        a = maps[pairs - 1, t, 0:8, :]
        bu = maps[pairs - 1, t, 8:16, :]
        bv = maps[pairs - 1, t, 16:24, :]
        for p in reversed(range(pairs - 1)):
            factor = maps[p, t, 0:8, :]
            a = factor * a
            bu = factor * bu + maps[p, t, 8:16, :]
            bv = factor * bv + maps[p, t, 16:24, :]
        share = 1.0 / (1.0 - a)
        u = bu * share
        v = bv * share
        for p in reversed(range(pairs)):
            carries[p, t, 0:8, :] = u
            carries[p, t, 8:16, :] = v
            if p:
                factor = maps[p, t, 0:8, :]
                u = factor * u + maps[p, t, 8:16, :]
                v = factor * v + maps[p, t, 16:24, :]


def add_tiles(gradient, tile_map, row, column):
    lanes = lax.broadcasted_iota(jnp.int32, (1, 128), 1)
    row = jnp.clip(row, 0, tile_map.shape[0] - 1)
    for j in range(tile_map.shape[1]):
        amount = jnp.sum(column[:, j * TILE : (j + 1) * TILE], axis=1, keepdims=True)
        gradient = gradient + jnp.where(lanes == tile_map[row, j], amount, 0.0)
    return gradient


def spread_kernel(
    place, tile_map, carries, keep, following, near, far, inner,
    coarse, late, edge, partial, frame,
):
    strip, core = place_of(place)
    half, width = keep.shape[2:]
    rows = half + 2 * PAD
    first = (2 * strip + core) * half
    for t, (r, c) in enumerate(blocks(half, width)):
        for i in range(2):
            entering = carries[t, 8 * i : 8 * i + 8, :]
            mismatch = keep[1, 1 + i, r : r + 8, c : c + 128] - following[i, r : r + 8, c : c + 128]
            entering = keep[1, 0, r : r + 8, c : c + 128] * entering + mismatch
            coarse[1, i, r : r + 8, c : c + 128] = entering
            coarse[0, i, r : r + 8, c : c + 128] = (
                keep[0, 0, r : r + 8, c : c + 128] * entering
                + keep[0, 1 + i, r : r + 8, c : c + 128]
            )
    for i in range(2):
        late[i] = coarse[1, i]
        for k in range(2):
            row = PAD * (2 * k + i)
            edge[row : row + PAD, :] = coarse[k, i, at((half - PAD) * core, PAD), :]
    frame[: 2 * PAD, :] = jnp.zeros((2 * PAD, width), jnp.float32)
    frame[2 * PAD + half :, :] = jnp.zeros((2 * PAD, width), jnp.float32)
    above = jnp.zeros((8, width), jnp.float32)
    amid = jnp.zeros((8, width), jnp.float32)
    below = jnp.zeros((8, width), jnp.float32)
    for k in range(2):
        for b in range(half // 8):
            here = slice(8 * b, 8 * b + 8)
            u = coarse[k, 0, here, :]
            total = coarse[k, 1, here, :] + DT * u
            drop = inner[k, here, :] * total
            frame[2 * PAD + 8 * b : 2 * PAD + 8 * b + 8, :] = DT * drop
            weight = far[k, PAD + 8 * b : PAD + 8 * b + 8, :]
            amid = amid + near[k, here, :] * total
            amid = amid + weight * (total - (DT * DAMP) * drop + DT * u)
        for b in range(rows // 8):
            weight = DT * far[k, 8 * b : 8 * b + 8, :]
            spread = laplacian(frame, PAD + 8 * b) * weight
            if b == 0:
                above = above + spread
            elif b == rows // 8 - 1:
                below = below + spread
            else:
                amid = amid + spread
    above, amid, below = [jnp.sum(a, axis=0, keepdims=True) for a in (above, amid, below)]
    gradient = jnp.zeros((1, 128), jnp.float32)
    gradient = add_tiles(gradient, tile_map, (first + TILE - 1) // TILE - 1, above)
    gradient = add_tiles(gradient, tile_map, first // TILE, amid)
    gradient = add_tiles(gradient, tile_map, (first + half) // TILE, below)
    partial[...] = jnp.broadcast_to(gradient, partial.shape)


def pass_kernel(place, coarse, edge, preceding, forward_edge, share, out):
    strip, core = place_of(place)
    half = coarse.shape[2]
    for i in range(2):
        out[half * i : half * i + half, :] = coarse[1 - core, i]
        out[half * (2 + i) : half * (3 + i), :] = jnp.where(core == 0, coarse[0, i], preceding[i])
        row = 4 * half + PAD * i
        out[row : row + PAD, :] = edge[at(PAD * (2 * (1 - core) + i), PAD), :]
    out[4 * half + 2 * PAD : 4 * half + 3 * PAD, :] = forward_edge[4 * PAD :, :]
    out[4 * half + 3 * PAD :, :128] = jnp.broadcast_to(share[...], (PAD, 128))


def adjoint_kernel(
    strips,
    place, step, modulation, tile_map, coarse, edge, preceding, forward_edge, came, eps, share,
    adjoint_u, adjoint_v, gradient,
    frame, field, total, static, before,
):
    strip, core = place_of(place)
    rows, width = eps.shape
    half = rows // 2
    count = rows + 2 * PAD
    here = at(PAD + half * core, half)
    there = at(PAD + half * (1 - core), half)
    near = at((rows + PAD) * core, PAD)
    far = at((rows + PAD) * (1 - core), PAD)
    for i, target in enumerate((field, total)):
        target[here, :] = coarse[core, i]
        target[there, :] = came[half * i : half * i + half, :]
        target[near, :] = edge[at(PAD * (2 * core + i), PAD), :]
        row = 4 * half + PAD * i
        target[far, :] = came[row : row + PAD, :]
        before[i, at(half * core, half), :] = jnp.where(core == 0, preceding[i], coarse[0, i])
        before[i, at(half * (1 - core), half), :] = came[half * (2 + i) : half * (3 + i), :]
    static[PAD : PAD + rows, :] = eps[...]
    static[near, :] = forward_edge[4 * PAD :, :]
    static[far, :] = came[4 * half + 2 * PAD : 4 * half + 3 * PAD, :]
    gradient[...] = share[...] + came[4 * half + 3 * PAD : 4 * half + 3 * PAD + 1, :128]

    inside = [strip > 0] + [None] * (rows // 8) + [strip < strips - 1]
    depth = depth_blocks(modulation, tile_map, strip * rows, rows)
    start = jnp.full((1, 1), step[0].astype(jnp.float32))
    cosines = [cosine(start, level) for level in range(2)]
    for i in range(2):
        frame[i, :PAD, :] = jnp.zeros((PAD, width), jnp.float32)
        frame[i, PAD + count :, :] = jnp.zeros((PAD, width), jnp.float32)
    for b in range(count // 8):
        this = slice(8 * b, 8 * b + 8)
        steady = static[this, :]
        if inside[b] is not None:
            steady = jnp.where(inside[b], steady, 1.0)
            static[this, :] = steady
        inverse = 1.0 / (steady * (1.0 + depth[b] * cosines[1]))
        amount = total[this, :] + DT * field[this, :]
        drop = DT * inverse * amount
        frame[0, PAD + 8 * b : PAD + 8 * b + 8, :] = drop
        total[this, :] = amount - DAMP * drop
    for b in range(count // 8):
        this = slice(8 * b, 8 * b + 8)
        inverse = 1.0 / (static[this, :] * (1.0 + depth[b] * cosines[0]))
        u = field[this, :] + laplacian(frame.at[0], PAD + 8 * b)
        amount = total[this, :] + DT * u
        drop = DT * inverse * amount
        if inside[b] is not None:
            drop = jnp.where(inside[b], drop, 0.0)
        else:
            out = slice(8 * b - PAD, 8 * b - PAD + 8)
            adjoint_v[out, :] = amount - DAMP * drop - before[1, out, :]
            field[this, :] = u
        frame[1, PAD + 8 * b : PAD + 8 * b + 8, :] = drop
    for b in range(rows // 8):
        this = slice(8 * b, 8 * b + 8)
        u = field[PAD + 8 * b : PAD + 8 * b + 8, :] - before[0, this, :]
        adjoint_u[this, :] = u + laplacian(frame.at[1], 2 * PAD + 8 * b)


def shifted(array, axis, by):
    length = lax.axis_size(axis)
    return lax.ppermute(array, axis, [(i, (i + by) % length) for i in range(length)])


def swapped(edge):
    strips = lax.axis_size(STRIP)
    pairs = [(strips + i, i + 1) for i in range(strips - 1)]
    return lax.ppermute(edge, HALVES, pairs + [(b, a) for a, b in pairs])


def summed(copies, axes):
    copies = copies.reshape(copies.shape[0], 1, copies.shape[1])
    return jnp.sum(lax.all_to_all(copies, axes, 0, 0, tiled=True), axis=0)


def shards(forward_u, forward_v, permittivity, coarse_rate, modulation, tile_map, start_step):
    rows, width = permittivity.shape
    half = rows // 2
    strips = lax.axis_size(STRIP)
    slices = lax.axis_size(TM)
    pairs = lax.axis_size(CHIPS)
    tiles = half // 8 * (width // 128)
    held = tiles // pairs
    place = (2 * lax.axis_index(STRIP) + lax.axis_index(CORE)).astype(jnp.int32).reshape(1)
    inputs = [forward_u[0], forward_v[0], coarse_rate[0]]
    tail = PAD
    state = (2, half, width)

    (send,) = call(
        gather_kernel, [SMEM, SMEM] + [HBM] * 3, [(3 * (half + PAD) + tail, width)],
        [pltpu.SemaphoreType.DMA((3,))],
    )(place, start_step, *[pltpu.with_memory_space_constraint(field, pltpu.HBM) for field in inputs])
    came = shifted(send, CORE, 1)
    fields, early, edge = call(
        sort_kernel, [SMEM] + [VMEM] * 5,
        [(2, 3, half + PAD, width), state, (5 * PAD, width)],
    )(place, *inputs, permittivity, came)
    following = shifted(early, CHIPS, -1)
    forward_edge = swapped(edge)
    keep, near, far, inner = call(
        functools.partial(forward_kernel, slices, strips),
        [SMEM] * 4 + [VMEM] * 4,
        [(2, 3, half, width), state, (2, half + 2 * PAD, width), state],
        [(2, half + 4 * PAD, width), (half + 2 * PAD, width), (half + 2 * PAD, width)],
    )(place, start_step, modulation, tile_map, fields, permittivity, came, forward_edge)
    (maps,) = call(pair_kernel, [VMEM] * 2, [(tiles, 24, 128)])(keep, following)

    maps = lax.all_to_all(maps.reshape(pairs, held * 24, 128), CHIPS, 0, 0, tiled=True)
    (carries,) = call(cycle_kernel, [VMEM], [(pairs, held, 16, 128)])(
        maps.reshape(pairs, held, 24, 128)
    )
    carries = lax.all_to_all(carries.reshape(pairs, held * 16, 128), CHIPS, 0, 0, tiled=True)

    coarse, late, edge, partial = call(
        spread_kernel, [SMEM, SMEM] + [VMEM] * 6,
        [(2, 2, half, width), state, (4 * PAD, width), (lax.axis_size(ALL_CHIPS), 128)],
        [(half + 4 * PAD, width)],
    )(place, tile_map, carries.reshape(tiles, 16, 128), keep, following, near, far, inner)
    preceding = shifted(late, CHIPS, 1)
    edge = swapped(edge)
    total = summed(partial, ALL_CHIPS)
    (send,) = call(pass_kernel, [SMEM] + [VMEM] * 5, [(4 * half + 4 * PAD, width)])(
        place, coarse, edge, preceding, forward_edge, total
    )
    came = shifted(send, CORE, 1)
    adjoint_u, adjoint_v, total = call(
        functools.partial(adjoint_kernel, strips),
        [SMEM] * 4 + [VMEM] * 7,
        [(rows, width), (rows, width), (1, 128)],
        [
            (2, rows + 4 * PAD, width), (rows + 2 * PAD, width), (rows + 2 * PAD, width),
            (rows + 2 * PAD, width), (2, rows, width),
        ],
    )(
        place, start_step, modulation, tile_map, coarse, edge, preceding, forward_edge, came,
        permittivity, total,
    )
    depth_grad = total[0, : modulation.shape[0]]
    return (adjoint_u[None], adjoint_v[None], depth_grad)


def solution(mesh):
    torus = Mesh(
        mesh.devices.reshape(4, 8, 2, 2, 4), ("tm_0", "tm_1", "tm_2", "strip_0", "strip_1")
    )
    return on_torus(torus)


def on_torus(torus):
    placed = (
        P(TM, STRIP, None),
        P(TM, STRIP, None),
        P(STRIP, None),
        P(TM, STRIP, None),
        P(),
        P(),
        P(TM),
    )
    return jax.shard_map(
        shards,
        mesh=torus,
        in_specs=placed,
        out_specs=(P(TM, STRIP, None), P(TM, STRIP, None), P()),
        check_vma=False,
    )
```

```python
import functools

import jax
import jax.numpy as jnp
from jax import lax
from jax.experimental import pallas as pl
from jax.experimental.pallas import tpu as pltpu
from jax.sharding import Mesh
from jax.sharding import PartitionSpec as P

TILE = 128
PERIOD = 256
STRIP = ("strip_0", "strip_1")
TM = ("tm_0", "tm_1", "tm_2")
CHIPS = ("tm_0", "tm_1")
CORE = "tm_2"
PAD = 8

COEF = (-205.0 / 72.0, 8.0 / 5.0, -1.0 / 5.0, 8.0 / 315.0, -1.0 / 560.0)
DT = 0.4
DAMP = 0.1

INTERPRET = False
VMEM_LIMIT = 12 * 1024 * 1024

ALL_CHIPS = ("tm_0", "tm_1", "strip_0", "strip_1")
HALVES = (CORE,) + STRIP
VMEM = pl.BlockSpec(memory_space=pltpu.VMEM)
SMEM = pl.BlockSpec(memory_space=pltpu.SMEM)
HBM = pl.BlockSpec(memory_space=pltpu.HBM)


def held(shape):
    return pltpu.VMEM(shape, jnp.float32) if isinstance(shape, tuple) else shape


def call(kernel, ins, outs, scratch=()):
    return pl.pallas_call(
        kernel,
        in_specs=ins,
        out_specs=[VMEM] * len(outs),
        out_shape=[jax.ShapeDtypeStruct(shape, jnp.float32) for shape in outs],
        scratch_shapes=[held(shape) for shape in scratch],
        compiler_params=pltpu.CompilerParams(vmem_limit_bytes=VMEM_LIMIT),
        interpret=INTERPRET,
    )


def laplacian(frame, first):
    width = frame.shape[1]
    center = frame[first : first + 8, :]
    summed = (2.0 * COEF[0]) * center
    for j in range(1, 5):
        rows = frame[first + j : first + j + 8, :] + frame[first - j : first - j + 8, :]
        cols = pltpu.roll(center, j, 1) + pltpu.roll(center, width - j, 1)
        summed = summed + COEF[j] * (rows + cols)
    return summed


def depth_row(modulation, tile_map, row, count):
    row = jnp.clip(row, 0, tile_map.shape[0] - 1)
    parts = [
        jnp.full((count, TILE), modulation[tile_map[row, j]], jnp.float32)
        for j in range(tile_map.shape[1])
    ]
    return jnp.concatenate(parts, axis=1)


def depth_blocks(modulation, tile_map, first, rows):
    above = depth_row(modulation, tile_map, (first + TILE - 1) // TILE - 1, PAD)
    amid = depth_row(modulation, tile_map, first // TILE, PAD)
    below = depth_row(modulation, tile_map, (first + rows) // TILE, PAD)
    return [above] + [amid] * (rows // 8) + [below]


def cosine(step, level):
    offset = jnp.broadcast_to(step + float(level), (8, 128))
    return jnp.cos((2.0 * jnp.pi / PERIOD) * offset)[:1, :1]


def place_of(place):
    return place[0] // 2, place[0] % 2


def at(start, count):
    return pl.ds(pl.multiple_of(start, PAD), count)


def gather_kernel(place, step, u, v, rate, out, sems):
    _, core = place_of(place)
    count = u.shape[0] // 2 + PAD
    rows = at((count - 2 * PAD) * (1 - core), count)
    copies = [
        pltpu.make_async_copy(field.at[rows, :], out.at[pl.ds(count * i, count), :], sems.at[i])
        for i, field in enumerate((u, v, rate))
    ]
    for copy in copies:
        copy.start()
    tail = out.shape[0] - 3 * count
    out[3 * count :, :] = jnp.full((tail, out.shape[1]), step[0].astype(jnp.float32))
    for copy in copies:
        copy.wait()


def sort_kernel(place, u, v, rate, eps, came, state, early, edge):
    _, core = place_of(place)
    half = u.shape[0] // 2
    count = half + PAD
    rows = at((half - PAD) * core, count)
    for i, field in enumerate((u, v, rate)):
        state[core, i] = field[rows, :]
        state[1 - core, i] = came[count * i : count * i + count, :]
    for i in range(2):
        early[i] = state[0, i, at(PAD * core, half), :]
    for k in range(2):
        for i in range(2):
            row = PAD * (2 * k + i)
            edge[row : row + PAD, :] = state[k, i, at(half * core, PAD), :]
    edge[4 * PAD :, :] = eps[at((2 * half - PAD) * core, PAD), :]


def forward_kernel(
    slices, strips,
    place, step, modulation, tile_map, state, eps, came, edge,
    keep, near, far, inner,
    frame, speed, static,
):
    strip, core = place_of(place)
    half = eps.shape[0] // 2
    width = eps.shape[1]
    rows = half + 2 * PAD
    first = (2 * strip + core) * half
    inside = [first > 0] + [None] * (half // 8) + [first + half < strips * 2 * half]
    body = at(PAD * (1 - core), half + PAD)
    rim = at((half + PAD) * core, PAD)

    static[body, :] = eps[at((half - PAD) * core, half + PAD), :]
    static[rim, :] = edge[4 * PAD :, :]
    for b in (0, rows // 8 - 1):
        static[8 * b : 8 * b + 8, :] = jnp.where(inside[b], static[8 * b : 8 * b + 8, :], 1.0)
    depth = depth_blocks(modulation, tile_map, first, half)
    own = jnp.full((1, 1), step[0].astype(jnp.float32))
    other = came[3 * (half + PAD) : 3 * (half + PAD) + 1, :1]
    for i in range(2):
        frame[i, :PAD, :] = jnp.zeros((PAD, width), jnp.float32)
        frame[i, PAD + rows :, :] = jnp.zeros((PAD, width), jnp.float32)
    for k in range(2):
        start = jnp.where(core == k, own, other)
        cosines = [cosine(start, level) for level in range(2)]
        frame[0, at(PAD + PAD * (1 - core), half + PAD), :] = state[k, 0]
        frame[0, at(PAD + (half + PAD) * core, PAD), :] = edge[2 * PAD * k : 2 * PAD * k + PAD, :]
        speed[body, :] = state[k, 1]
        speed[rim, :] = edge[2 * PAD * k + PAD : 2 * PAD * k + 2 * PAD, :]
        for b in range(rows // 8):
            here = slice(8 * b, 8 * b + 8)
            there = slice(PAD + 8 * b, PAD + 8 * b + 8)
            steady = static[here, :]
            inverse = 1.0 / (steady * (1.0 + depth[b] * cosines[0]))
            v = speed[here, :]
            force = laplacian(frame.at[0], PAD + 8 * b) - DAMP * v
            pull = force * inverse
            weight = (cosines[0] * -DT) * pull * inverse * steady
            v = v + DT * pull
            u = frame[0, there, :] + DT * v
            if inside[b] is not None:
                weight = jnp.where(inside[b], weight, 0.0)
                u = jnp.where(inside[b], u, 0.0)
            else:
                speed[here, :] = v
            far[k, here, :] = weight
            frame[1, there, :] = u
        for b in range(half // 8):
            here = slice(8 * b, 8 * b + 8)
            outer = slice(PAD + 8 * b, PAD + 8 * b + 8)
            steady = static[outer, :]
            inverse = 1.0 / (steady * (1.0 + depth[1 + b] * cosines[1]))
            v = speed[outer, :]
            force = laplacian(frame.at[1], 2 * PAD + 8 * b) - DAMP * v
            pull = force * inverse
            near[k, here, :] = (cosines[1] * -DT) * pull * inverse * steady
            inner[k, here, :] = inverse
            v = v + DT * pull
            u = frame[1, 2 * PAD + 8 * b : 2 * PAD + 8 * b + 8, :] + DT * v
            rows_here = at(PAD * core + 8 * b, 8)
            keep[k, 0, here, :] = jnp.exp(-state[k, 2, rows_here, :] / slices)
            if k == 0:
                u = u - state[1, 0, rows_here, :]
                v = v - state[1, 1, rows_here, :]
            keep[k, 1, here, :] = u
            keep[k, 2, here, :] = v


def blocks(rows, width):
    return [(8 * i, 128 * j) for i in range(rows // 8) for j in range(width // 128)]


def pair_kernel(keep, following, maps):
    half, width = keep.shape[2:]
    for t, (r, c) in enumerate(blocks(half, width)):
        factor = keep[0, 0, r : r + 8, c : c + 128]
        maps[t, 0:8, :] = factor * keep[1, 0, r : r + 8, c : c + 128]
        for i in range(2):
            mismatch = keep[1, 1 + i, r : r + 8, c : c + 128] - following[i, r : r + 8, c : c + 128]
            maps[t, 8 * (1 + i) : 8 * (2 + i), :] = (
                factor * mismatch + keep[0, 1 + i, r : r + 8, c : c + 128]
            )


def cycle_kernel(maps, carries):
    pairs, held = maps.shape[:2]
    for t in range(held):
        a = maps[pairs - 1, t, 0:8, :]
        bu = maps[pairs - 1, t, 8:16, :]
        bv = maps[pairs - 1, t, 16:24, :]
        for p in reversed(range(pairs - 1)):
            factor = maps[p, t, 0:8, :]
            a = factor * a
            bu = factor * bu + maps[p, t, 8:16, :]
            bv = factor * bv + maps[p, t, 16:24, :]
        share = 1.0 / (1.0 - a)
        u = bu * share
        v = bv * share
        for p in reversed(range(pairs)):
            carries[p, t, 0:8, :] = u
            carries[p, t, 8:16, :] = v
            if p:
                factor = maps[p, t, 0:8, :]
                u = factor * u + maps[p, t, 8:16, :]
                v = factor * v + maps[p, t, 16:24, :]


def add_tiles(gradient, tile_map, row, column):
    lanes = lax.broadcasted_iota(jnp.int32, (1, 128), 1)
    row = jnp.clip(row, 0, tile_map.shape[0] - 1)
    for j in range(tile_map.shape[1]):
        amount = jnp.sum(column[:, j * TILE : (j + 1) * TILE], axis=1, keepdims=True)
        gradient = gradient + jnp.where(lanes == tile_map[row, j], amount, 0.0)
    return gradient


def spread_kernel(
    place, tile_map, carries, keep, following, near, far, inner,
    coarse, late, edge, partial, frame,
):
    strip, core = place_of(place)
    half, width = keep.shape[2:]
    rows = half + 2 * PAD
    first = (2 * strip + core) * half
    for t, (r, c) in enumerate(blocks(half, width)):
        for i in range(2):
            entering = carries[t, 8 * i : 8 * i + 8, :]
            mismatch = keep[1, 1 + i, r : r + 8, c : c + 128] - following[i, r : r + 8, c : c + 128]
            entering = keep[1, 0, r : r + 8, c : c + 128] * entering + mismatch
            coarse[1, i, r : r + 8, c : c + 128] = entering
            coarse[0, i, r : r + 8, c : c + 128] = (
                keep[0, 0, r : r + 8, c : c + 128] * entering
                + keep[0, 1 + i, r : r + 8, c : c + 128]
            )
    for i in range(2):
        late[i] = coarse[1, i]
        for k in range(2):
            row = PAD * (2 * k + i)
            edge[row : row + PAD, :] = coarse[k, i, at((half - PAD) * core, PAD), :]
    frame[: 2 * PAD, :] = jnp.zeros((2 * PAD, width), jnp.float32)
    frame[2 * PAD + half :, :] = jnp.zeros((2 * PAD, width), jnp.float32)
    above = jnp.zeros((8, width), jnp.float32)
    amid = jnp.zeros((8, width), jnp.float32)
    below = jnp.zeros((8, width), jnp.float32)
    for k in range(2):
        for b in range(half // 8):
            here = slice(8 * b, 8 * b + 8)
            u = coarse[k, 0, here, :]
            total = coarse[k, 1, here, :] + DT * u
            drop = inner[k, here, :] * total
            frame[2 * PAD + 8 * b : 2 * PAD + 8 * b + 8, :] = DT * drop
            weight = far[k, PAD + 8 * b : PAD + 8 * b + 8, :]
            amid = amid + near[k, here, :] * total
            amid = amid + weight * (total - (DT * DAMP) * drop + DT * u)
        for b in range(rows // 8):
            weight = DT * far[k, 8 * b : 8 * b + 8, :]
            spread = laplacian(frame, PAD + 8 * b) * weight
            if b == 0:
                above = above + spread
            elif b == rows // 8 - 1:
                below = below + spread
            else:
                amid = amid + spread
    above, amid, below = [jnp.sum(a, axis=0, keepdims=True) for a in (above, amid, below)]
    gradient = jnp.zeros((1, 128), jnp.float32)
    gradient = add_tiles(gradient, tile_map, (first + TILE - 1) // TILE - 1, above)
    gradient = add_tiles(gradient, tile_map, first // TILE, amid)
    gradient = add_tiles(gradient, tile_map, (first + half) // TILE, below)
    partial[...] = jnp.broadcast_to(gradient, partial.shape)


def pass_kernel(place, coarse, edge, preceding, forward_edge, share, out):
    _, core = place_of(place)
    half = coarse.shape[2]
    for i in range(2):
        out[half * i : half * i + half, :] = coarse[1 - core, i]
        out[half * (2 + i) : half * (3 + i), :] = jnp.where(core == 0, coarse[0, i], preceding[i])
        row = 4 * half + PAD * i
        out[row : row + PAD, :] = edge[at(PAD * (2 * (1 - core) + i), PAD), :]
    out[4 * half + 2 * PAD : 4 * half + 3 * PAD, :] = forward_edge[4 * PAD :, :]
    out[4 * half + 3 * PAD :, :128] = jnp.broadcast_to(share[...], (PAD, 128))


def adjoint_kernel(
    strips,
    place, step, modulation, tile_map, coarse, edge, preceding, forward_edge, came, eps, share,
    adjoint_u, adjoint_v, gradient,
    frame, field, total, static, before,
):
    strip, core = place_of(place)
    rows, width = eps.shape
    half = rows // 2
    count = rows + 2 * PAD
    here = at(PAD + half * core, half)
    there = at(PAD + half * (1 - core), half)
    near = at((rows + PAD) * core, PAD)
    far = at((rows + PAD) * (1 - core), PAD)
    for i, target in enumerate((field, total)):
        target[here, :] = coarse[core, i]
        target[there, :] = came[half * i : half * i + half, :]
        target[near, :] = edge[at(PAD * (2 * core + i), PAD), :]
        row = 4 * half + PAD * i
        target[far, :] = came[row : row + PAD, :]
        before[i, at(half * core, half), :] = jnp.where(core == 0, preceding[i], coarse[0, i])
        before[i, at(half * (1 - core), half), :] = came[half * (2 + i) : half * (3 + i), :]
    static[PAD : PAD + rows, :] = eps[...]
    static[near, :] = forward_edge[4 * PAD :, :]
    static[far, :] = came[4 * half + 2 * PAD : 4 * half + 3 * PAD, :]
    gradient[...] = share[...] + came[4 * half + 3 * PAD : 4 * half + 3 * PAD + 1, :128]

    inside = [strip > 0] + [None] * (rows // 8) + [strip < strips - 1]
    depth = depth_blocks(modulation, tile_map, strip * rows, rows)
    start = jnp.full((1, 1), step[0].astype(jnp.float32))
    cosines = [cosine(start, level) for level in range(2)]
    for i in range(2):
        frame[i, :PAD, :] = jnp.zeros((PAD, width), jnp.float32)
        frame[i, PAD + count :, :] = jnp.zeros((PAD, width), jnp.float32)
    for b in range(count // 8):
        this = slice(8 * b, 8 * b + 8)
        steady = static[this, :]
        if inside[b] is not None:
            steady = jnp.where(inside[b], steady, 1.0)
            static[this, :] = steady
        inverse = 1.0 / (steady * (1.0 + depth[b] * cosines[1]))
        amount = total[this, :] + DT * field[this, :]
        drop = DT * inverse * amount
        frame[0, PAD + 8 * b : PAD + 8 * b + 8, :] = drop
        total[this, :] = amount - DAMP * drop
    for b in range(count // 8):
        this = slice(8 * b, 8 * b + 8)
        inverse = 1.0 / (static[this, :] * (1.0 + depth[b] * cosines[0]))
        u = field[this, :] + laplacian(frame.at[0], PAD + 8 * b)
        amount = total[this, :] + DT * u
        drop = DT * inverse * amount
        if inside[b] is not None:
            drop = jnp.where(inside[b], drop, 0.0)
        else:
            out = slice(8 * b - PAD, 8 * b - PAD + 8)
            adjoint_v[out, :] = amount - DAMP * drop - before[1, out, :]
            field[this, :] = u
        frame[1, PAD + 8 * b : PAD + 8 * b + 8, :] = drop
    for b in range(rows // 8):
        this = slice(8 * b, 8 * b + 8)
        u = field[PAD + 8 * b : PAD + 8 * b + 8, :] - before[0, this, :]
        adjoint_u[this, :] = u + laplacian(frame.at[1], 2 * PAD + 8 * b)


def shifted(array, axis, by):
    length = lax.axis_size(axis)
    return lax.ppermute(array, axis, [(i, (i + by) % length) for i in range(length)])


def swapped(edge):
    strips = lax.axis_size(STRIP)
    pairs = [(strips + i, i + 1) for i in range(strips - 1)]
    return lax.ppermute(edge, HALVES, pairs + [(b, a) for a, b in pairs])


def summed(copies, axes):
    copies = copies.reshape(copies.shape[0], 1, copies.shape[1])
    return jnp.sum(lax.all_to_all(copies, axes, 0, 0, tiled=True), axis=0)


def shards(forward_u, forward_v, permittivity, coarse_rate, modulation, tile_map, start_step):
    rows, width = permittivity.shape
    half = rows // 2
    strips = lax.axis_size(STRIP)
    slices = lax.axis_size(TM)
    pairs = lax.axis_size(CHIPS)
    tiles = half // 8 * (width // 128)
    held = tiles // pairs
    place = (2 * lax.axis_index(STRIP) + lax.axis_index(CORE)).astype(jnp.int32).reshape(1)
    inputs = [forward_u[0], forward_v[0], coarse_rate[0]]
    tail = PAD
    state = (2, half, width)

    (send,) = call(
        gather_kernel, [SMEM, SMEM] + [HBM] * 3, [(3 * (half + PAD) + tail, width)],
        [pltpu.SemaphoreType.DMA((3,))],
    )(place, start_step, *[pltpu.with_memory_space_constraint(field, pltpu.HBM) for field in inputs])
    came = shifted(send, CORE, 1)
    fields, early, edge = call(
        sort_kernel, [SMEM] + [VMEM] * 5,
        [(2, 3, half + PAD, width), state, (5 * PAD, width)],
    )(place, *inputs, permittivity, came)
    following = shifted(early, CHIPS, -1)
    forward_edge = swapped(edge)
    keep, near, far, inner = call(
        functools.partial(forward_kernel, slices, strips),
        [SMEM] * 4 + [VMEM] * 4,
        [(2, 3, half, width), state, (2, half + 2 * PAD, width), state],
        [(2, half + 4 * PAD, width), (half + 2 * PAD, width), (half + 2 * PAD, width)],
    )(place, start_step, modulation, tile_map, fields, permittivity, came, forward_edge)
    (maps,) = call(pair_kernel, [VMEM] * 2, [(tiles, 24, 128)])(keep, following)

    maps = lax.all_to_all(maps.reshape(pairs, held * 24, 128), CHIPS, 0, 0, tiled=True)
    (carries,) = call(cycle_kernel, [VMEM], [(pairs, held, 16, 128)])(
        maps.reshape(pairs, held, 24, 128)
    )
    carries = lax.all_to_all(carries.reshape(pairs, held * 16, 128), CHIPS, 0, 0, tiled=True)

    coarse, late, edge, partial = call(
        spread_kernel, [SMEM, SMEM] + [VMEM] * 6,
        [(2, 2, half, width), state, (4 * PAD, width), (lax.axis_size(ALL_CHIPS), 128)],
        [(half + 4 * PAD, width)],
    )(place, tile_map, carries.reshape(tiles, 16, 128), keep, following, near, far, inner)
    total = summed(partial, ALL_CHIPS)
    preceding = shifted(late, CHIPS, 1)
    edge = swapped(edge)
    (send,) = call(pass_kernel, [SMEM] + [VMEM] * 5, [(4 * half + 4 * PAD, width)])(
        place, coarse, edge, preceding, forward_edge, total
    )
    came = shifted(send, CORE, 1)
    adjoint_u, adjoint_v, total = call(
        functools.partial(adjoint_kernel, strips),
        [SMEM] * 4 + [VMEM] * 7,
        [(rows, width), (rows, width), (1, 128)],
        [
            (2, rows + 4 * PAD, width), (rows + 2 * PAD, width), (rows + 2 * PAD, width),
            (rows + 2 * PAD, width), (2, rows, width),
        ],
    )(
        place, start_step, modulation, tile_map, coarse, edge, preceding, forward_edge, came,
        permittivity, total,
    )
    depth_grad = total[0, : modulation.shape[0]]
    return (adjoint_u[None], adjoint_v[None], depth_grad)


def solution(mesh):
    torus = Mesh(
        mesh.devices.reshape(4, 8, 2, 2, 4), ("tm_0", "tm_1", "tm_2", "strip_0", "strip_1")
    )
    return on_torus(torus)


def on_torus(torus):
    placed = (
        P(TM, STRIP, None),
        P(TM, STRIP, None),
        P(STRIP, None),
        P(TM, STRIP, None),
        P(),
        P(),
        P(TM),
    )
    return jax.shard_map(
        shards,
        mesh=torus,
        in_specs=placed,
        out_specs=(P(TM, STRIP, None), P(TM, STRIP, None), P()),
        check_vma=False,
    )
```
